32 devices in a mesh: cls: 8 (over z, x), dp: 4 (over y, core).
Axes of the slice: x: 2, y: 2, z: 4, core: 2. Of those that a mesh axis runs over, the one named last changes fastest.
Arguments:
- embeddings: bfloat16 [256, 512], P(('dp', 'cls')), parts along dimension 0, may hold values from -4.4194174 to 4.4194174
- labels: int32 [256], P(('dp', 'cls')), parts along dimension 0, may hold values from 0 to 32767
- centers: bfloat16 [131072, 512], P(('dp', 'cls')), parts along dimension 0, may hold values from -3.0935922 to 3.0935922
Outputs:
- losses: float32 [256], P(('dp', 'cls')), parts along dimension 0
- emb_grad: float32 [256, 512], P(('dp', 'cls')), parts along dimension 0
- center_grad: float32 [131072, 512], P(('dp', 'cls')), parts along dimension 0
The draws below stay inside these ranges and needn't reach their ends.
There are 4 independent parts, one for each index of `dp`. The reference program is written for one: setup_inputs(seed, part) draws one part's arguments, and reference() takes and returns one part's arrays. A program takes and returns all parts, laid end to end along the dimension named above; each array names one. Nothing has to cross between parts.
All inputs are finite; a program needn't handle non-finite values.
Results may differ from the reference program's by a relative error of at most 0.0042.
Values may be sent and summed in bfloat16 or wider, within the bound.
A program may use at most 64 MiB of HBM per device.

```python
import math
import jax
import jax.numpy as jnp
from jax import lax

D = 512
C_DEV = 4096
CLASSES = 32768
BATCH = 64
N_CLS = 8


def shared_direction(key):
    return jnp.clip(jax.random.normal(jax.random.fold_in(key, 101), (D,), jnp.float32), -3.0, 3.0)


def noisy_rows(key, row_count):
    noise_key = jax.random.fold_in(key, 11)
    scale_key = jax.random.fold_in(key, 12)
    noise_part = jnp.clip(jax.random.normal(noise_key, (row_count, D), jnp.float32), -5.0, 5.0)
    scales = jnp.exp(jax.random.uniform(scale_key, (row_count, 1), jnp.float32, 0.0, math.log(10.0)))
    return (noise_part, scales)


def draw_embeddings(key, part):
    direction = shared_direction(key)
    noise_part, scales = noisy_rows(jax.random.fold_in(key, 21), BATCH)
    lean_share = 0.3
    values = scales * (noise_part + lean_share * direction[None, :]) / math.sqrt(D)
    return values.astype(jnp.bfloat16)


def draw_centers(key, part):
    direction = shared_direction(key)
    noise_part, scales = noisy_rows(jax.random.fold_in(key, 31), CLASSES)
    ramp_share = 0.06
    ramp = jnp.arange(CLASSES, dtype=jnp.float32) / max(CLASSES - 1, 1) * ramp_share
    values = scales * (noise_part + ramp[:, None] * direction[None, :]) / math.sqrt(D)
    return values.astype(jnp.bfloat16)


def place_ends(entries, key, least, high):
    longest = entries.shape.index(max(entries.shape))
    spots = []
    for shift in (0, 1):
        where = [jax.random.randint(jax.random.fold_in(key, axis), (), 0, length) for axis, length in enumerate(entries.shape)]
        where[longest] = (where[longest] + shift) % entries.shape[longest]
        spots.append(tuple(where))
    return entries.at[spots[0]].set(least).at[spots[1]].set(high)


def setup_inputs(seed: int = 0, part: int = 0) -> dict:
    streams_of = jax.random.split(jax.random.key(seed), 4)
    part_splits = jax.random.split(jax.random.fold_in(streams_of[3], part), 4)
    embeddings = draw_embeddings(jax.random.fold_in(jax.random.fold_in(streams_of[3], part), 71), part)
    labels = place_ends(jax.random.randint(part_splits[1], (BATCH,), 0, CLASSES), jax.random.fold_in(part_splits[1], 1), 0, CLASSES - 1).astype(jnp.int32)
    centers = draw_centers(jax.random.fold_in(jax.random.fold_in(streams_of[3], part), 71), part)
    return dict(embeddings=embeddings, labels=labels, centers=centers)


logit_scale = 64.0
margin_cosine = math.cos(0.5)
margin_sine = math.sin(0.5)
sine_soften = 0.04
norm_eps = 1e-06

def unit_rows(values):
    widened = values.astype(jnp.float32)
    inverse = lax.rsqrt(lax.optimization_barrier(jnp.sum(widened * widened, axis=1, keepdims=True)) + norm_eps)
    normed = widened * inverse
    return (inverse, normed, normed.astype(jnp.bfloat16))

def score_block(rows_hat, rows_label, center_block, class_base):
    cosine = jnp.dot(rows_hat, center_block.T, preferred_element_type=jnp.float32)
    local_col = rows_label - class_base
    is_owned = (local_col >= 0) & (local_col < center_block.shape[0])
    column = lax.broadcasted_iota(jnp.int32, cosine.shape, 1)
    target_mask = column == local_col[:, None]
    target_cos = lax.optimization_barrier(jnp.sum(jnp.where(target_mask, cosine, 0.0), axis=1))
    target_sine = jnp.sqrt(1.0 + sine_soften - target_cos * target_cos)
    shifted = target_cos * margin_cosine - target_sine * margin_sine
    slopes = margin_cosine + margin_sine * target_cos / target_sine
    logits = jnp.where(target_mask, logit_scale * shifted[:, None], logit_scale * cosine)
    exp_terms = jnp.exp(logits - logit_scale)
    row_total = lax.optimization_barrier(jnp.sum(exp_terms, axis=1))
    weighted = (logit_scale * exp_terms * jnp.where(target_mask, slopes[:, None], 1.0)).astype(jnp.bfloat16)
    target = jnp.where(is_owned, logit_scale * shifted, 0.0)
    columns = jnp.where(is_owned, local_col, -1).astype(jnp.int32)
    return (weighted, row_total, target, columns, jnp.where(is_owned, slopes, 0.0))

def row_term(weighted, center_block, totals, columns, slopes):
    product = jnp.dot(weighted, center_block, preferred_element_type=jnp.float32)
    picked = jnp.take(center_block, jnp.clip(columns, 0, center_block.shape[0] - 1), axis=0).astype(jnp.float32)
    return product / totals[:, None] - (logit_scale * slopes)[:, None] * picked

def class_term(weighted, scaled, rows_hat, columns, slopes, class_count):
    product = lax.dot_general(weighted, scaled, (((0,), (0,)), ((), ())), preferred_element_type=jnp.float32)
    drop_index = jnp.where(columns >= 0, columns, class_count).astype(jnp.int32)
    updates = -(logit_scale * slopes)[:, None] * rows_hat.astype(jnp.float32)
    return product.at[drop_index].add(updates, mode='drop')

def reference(embeddings, labels, centers):
    inv_x, units_x, emb_hat = unit_rows(embeddings)
    inv_w, units_w, center_hat = unit_rows(centers)
    hat_blocks = center_hat.reshape(N_CLS, C_DEV, D)
    starts = jnp.arange(N_CLS, dtype=jnp.int32) * C_DEV
    zero_rows = jnp.zeros((BATCH,), jnp.float32)

    def forward(carry, block_item):
        center_block, class_base = block_item
        weighted, row_total, target, columns, slopes = score_block(emb_hat, labels, center_block, class_base)
        return ((carry[0] + row_total, carry[1] + target), None)
    (totals, targets), _ = lax.scan(forward, (zero_rows, zero_rows), (hat_blocks, starts))
    losses = jnp.log(totals) + logit_scale - targets
    scaled = (emb_hat.astype(jnp.float32) / totals[:, None]).astype(jnp.bfloat16)

    def backward(row_sums, block_item):
        center_block, class_base = block_item
        weighted, row_total, target, columns, slopes = score_block(emb_hat, labels, center_block, class_base)
        row_sums = row_sums + row_term(weighted, center_block, totals, columns, slopes)
        return (row_sums, class_term(weighted, scaled, emb_hat, columns, slopes, C_DEV))
    grad_hat_x, grad_blocks = lax.scan(backward, jnp.zeros((BATCH, D), jnp.float32), (hat_blocks, starts))
    grad_hat_w = grad_blocks.reshape(CLASSES, D)
    emb_grad = inv_x * (grad_hat_x - units_x * lax.optimization_barrier(jnp.sum(units_x * grad_hat_x, axis=1, keepdims=True)))
    center_grad = inv_w * (grad_hat_w - units_w * lax.optimization_barrier(jnp.sum(units_w * grad_hat_w, axis=1, keepdims=True)))
    return (losses, emb_grad, center_grad)
```

```python
import functools
import math

import jax
import jax.numpy as jnp
from jax import lax
from jax.experimental import pallas as pl
from jax.experimental.pallas import tpu as pltpu
from jax.sharding import PartitionSpec as P

logit_scale = 64.0
margin_cosine = math.cos(0.5)
margin_sine = math.sin(0.5)
sine_soften = 0.04
norm_eps = 1e-06
lanes = 128
never = -1e30
log2_e = math.log2(math.e)
MESH = pl.DeviceIdType.MESH
f32 = jnp.float32
bf16 = jnp.bfloat16


def iota(shape, dim):
    return lax.broadcasted_iota(jnp.int32, shape, dim)


def largest_tile(count, limit):
    tile = limit
    while count % tile:
        tile //= 2
    return tile


def partner(me, n, k):
    if n & (n - 1):
        return lax.rem(me + k, n)
    bit, other = 1, me
    while bit < n:
        if k & bit:
            other = other + bit * (1 - 2 * lax.rem(me // bit, 2))
        bit *= 2
    return other


def gradient_tile(lhs_ref, inv_ref, centers_ref, rhs_ref, at):
    width = centers_ref.shape[1]
    repeat = width // lanes
    inverse = inv_ref[at, :]
    centers = centers_ref[at, :].astype(f32)
    lhs = lhs_ref[at, :]
    if rhs_ref.shape[1] > width:
        both = jnp.dot(lhs, rhs_ref[...], preferred_element_type=f32)
        grad = both[:, :width]
        back = both[:, width:] * (inverse * inverse)
    else:
        grad = jnp.dot(jnp.concatenate([lhs, lhs], axis=1), rhs_ref[...], preferred_element_type=f32)
        along = jnp.sum(centers * grad, axis=1, keepdims=True)
        back = along * (inverse * inverse * inverse)
    return (
        jnp.concatenate([inverse] * repeat, axis=1) * grad
        - jnp.concatenate([back] * repeat, axis=1) * centers
    )


def exchange_kernel(
    n,
    head_tile,
    labels_hbm,
    emb_hbm,
    centers_ref,
    cbuf,
    lhs_ref,
    inv_ref,
    rhs_ref,
    fin_ref,
    col_ref,
    head_ref,
    hat,
    emb_ref,
    labels_ref,
    xall,
    lall,
    stat,
    stat_in,
    part,
    part_in,
    colst,
    load_sem,
    small_sem,
    x_send,
    x_recv,
    l_send,
    l_recv,
    s_send,
    s_recv,
    p_send,
    p_recv,
):
    me = lax.axis_index("cls")
    own, width = emb_ref.shape
    count = cbuf.shape[0]
    batch = n * own
    wide = 2 * batch
    fused = rhs_ref.shape[1] > width
    peers = [partner(me, n, k) for k in range(n - 1, 0, -1)]

    barrier = pltpu.get_barrier_semaphore()
    for peer in peers:
        pl.semaphore_signal(barrier, inc=1, device_id={"cls": peer}, device_id_type=MESH)

    small = [
        pltpu.make_async_copy(labels_hbm, labels_ref, small_sem.at[0]),
        pltpu.make_async_copy(emb_hbm, emb_ref, small_sem.at[1]),
    ]
    for copy in small:
        copy.start()
    load = largest_tile(count, 512)
    loads = []
    for k in range(count // load):
        copy = pltpu.make_async_copy(
            centers_ref.at[pl.ds(k * load, load)], cbuf.at[pl.ds(k * load, load)], load_sem.at[k]
        )
        copy.start()
        loads.append(copy)

    for copy in small:
        copy.wait()
    lane = iota((1, wide), 1)
    first = lane - me * own
    label_row = jnp.zeros((1, wide), jnp.int32)
    for i in range(own):
        label_row = jnp.where((first == i) | (first == batch + i), labels_ref[i], label_row)
    lall[me] = label_row
    x = emb_ref[...].astype(f32)
    xall[me] = (x * lax.rsqrt(jnp.sum(x * x, axis=1, keepdims=True) + norm_eps)).astype(bf16)

    def remote(src, dst, send, recv, peer):
        return pltpu.make_async_remote_copy(
            src_ref=src,
            dst_ref=dst,
            send_sem=send,
            recv_sem=recv,
            device_id={"cls": peer},
            device_id_type=MESH,
        )

    pl.semaphore_wait(barrier, n - 1)
    x_copies, l_copies = [], []
    for step, peer in enumerate(peers):
        copy = remote(xall.at[me], xall.at[me], x_send.at[step], x_recv.at[step], peer)
        copy.start()
        x_copies.append(copy)
        copy = remote(lall.at[me], lall.at[me], l_send.at[step], l_recv.at[step], peer)
        copy.start()
        l_copies.append(copy)

    sub = largest_tile(load, 64)
    for k in range(count // load):
        loads[k].wait()

        def norm(i, carry):
            at = pl.ds(pl.multiple_of(k * load + i * sub, sub), sub)
            c = cbuf[at, :].astype(f32)
            inverse = lax.rsqrt(jnp.sum(c * c, axis=1, keepdims=True) + norm_eps)
            inv_ref[at, :] = jnp.broadcast_to(inverse, (sub, lanes))
            hat[at, :] = (c * inverse).astype(bf16)
            return carry

        lax.fori_loop(0, load // sub, norm, 0, unroll=load // sub)

    for copy in x_copies + l_copies:
        copy.wait()

    x_hat = jnp.concatenate([xall[j] for j in range(n)], axis=0)
    x_both = jnp.concatenate([x_hat, x_hat], axis=0)
    label_row = lall[0]
    for j in range(1, n):
        label_row = label_row + lall[j]
    label_row = label_row - me * count
    bias = jnp.where(lane < batch, math.log2(logit_scale) - logit_scale * log2_e, never)
    one_hot_value = jnp.where(lane < batch, 0.0, 1.0)

    tile = largest_tile(count, 512 if wide <= 128 else 128)

    def score(k, sums):
        at = pl.ds(pl.multiple_of(k * tile, tile), tile)
        cosine = lax.dot_general(
            hat[at, :], x_both, (((1,), (1,)), ((), ())), preferred_element_type=f32
        )
        mask = iota((tile, wide), 0) == (label_row - k * tile)
        exps = jnp.exp2((logit_scale * log2_e) * cosine + bias)
        values = jnp.where(mask, one_hot_value, exps)
        products = values * cosine
        left = lane < batch
        lhs_ref[at, :wide] = values.astype(bf16)
        if fused:
            lhs_ref[at, wide:] = jnp.where(left, products, values).astype(bf16)
        counted = jnp.where(left, values, products)
        return sums + jnp.sum(counted.reshape(tile // 8, 8, wide), axis=0)

    sums = lax.fori_loop(
        0, count // tile, score, jnp.zeros((8, wide), f32), unroll=count // tile if fused else 1
    )
    stat[...] = jnp.sum(sums, axis=0, keepdims=True)
    s_copies = []
    for step, peer in enumerate(peers):
        copy = remote(stat, stat_in.at[step], s_send.at[step], s_recv.at[step], peer)
        copy.start()
        s_copies.append(copy)

    summed = lax.dot_general(
        lhs_ref[:, :wide], hat[...], (((0,), (0,)), ((), ())), preferred_element_type=f32
    )
    for j in range(n):
        part[j] = jnp.concatenate(
            [summed[j * own : (j + 1) * own], summed[batch + j * own : batch + (j + 1) * own]],
            axis=0,
        ).astype(bf16)
    p_copies = []
    for step, peer in enumerate(peers):
        copy = remote(part.at[peer], part_in.at[step], p_send.at[step], p_recv.at[step], peer)
        copy.start()
        p_copies.append(copy)

    for copy in s_copies:
        copy.wait()
    sums = stat[...]
    for step in range(n - 1):
        sums = sums + stat_in[step]
    others = sums * (1.0 / logit_scale)
    target_cos = jnp.concatenate([sums[:, batch:], sums[:, :batch]], axis=1)
    target_sine = jnp.sqrt(1.0 + sine_soften - target_cos * target_cos)
    shifted = target_cos * margin_cosine - target_sine * margin_sine
    slope = margin_cosine + margin_sine * target_cos / target_sine
    label_exp = jnp.exp(logit_scale * shifted - logit_scale)
    totals = others + label_exp
    label_weight = (logit_scale * label_exp * slope).astype(bf16).astype(f32)
    losses = jnp.log(totals) + logit_scale - logit_scale * shifted
    stack_row = iota((lanes, wide), 0)
    stack = jnp.where(
        stack_row == 0,
        totals,
        jnp.where(
            stack_row == 1,
            slope,
            jnp.where(
                stack_row == 2, label_weight, jnp.where(stack_row == 3, losses, target_cos)
            ),
        ),
    )
    columns = stack.T
    colst[...] = columns[:batch]
    total_col = columns[:batch, 0:1]
    slope_col = columns[:batch, 1:2]
    weight_col = columns[:batch, 2:3]
    x_wide = x_hat.astype(f32)
    scaled = (x_wide / total_col).astype(bf16)
    label_term = weight_col * scaled.astype(f32) - (logit_scale * slope_col) * x_wide
    high = label_term.astype(bf16)
    low = (label_term - high.astype(f32)).astype(bf16)
    rhs_ref[:, :width] = jnp.concatenate([scaled, high, jnp.zeros_like(high), low], axis=0)
    if fused:
        inverse = 1.0 / total_col
        dot = (weight_col * inverse - logit_scale * slope_col) * columns[:batch, 4:5]
        dot_high = dot.astype(bf16)
        dot_low = (dot - dot_high.astype(f32)).astype(bf16)
        rhs_ref[:, width:] = jnp.broadcast_to(
            jnp.concatenate([jnp.zeros_like(dot_high), dot_high, inverse.astype(bf16), dot_low], axis=0),
            (4 * batch, lanes),
        )
    col_ref[...] = colst[pl.ds(pl.multiple_of(me * own, own), own), :]
    for k in range(head_ref.shape[0] // head_tile):
        at = pl.ds(k * head_tile, head_tile)
        head_ref[at, :] = gradient_tile(lhs_ref, inv_ref, cbuf, rhs_ref, at)

    for copy in p_copies:
        copy.wait()
    mine = part[me].astype(f32)
    for step in range(n - 1):
        mine = mine + part_in[step].astype(f32)
    fin_ref[...] = mine


def gradient_kernel(
    tile,
    lhs_ref,
    inv_ref,
    centers_ref,
    rhs_ref,
    emb_ref,
    fin_ref,
    col_ref,
    head_ref,
    loss_hbm,
    emb_grad_hbm,
    grad_hbm,
    loss_buf,
    emb_grad_buf,
    grad_buf,
    sems,
):
    own, width = emb_ref.shape
    count = lhs_ref.shape[0]
    steps = count // tile
    head = head_ref.shape[0] // tile
    stores = []
    for k in range(head):
        at = pl.ds(k * tile, tile)
        copy = pltpu.make_async_copy(head_ref.at[at], grad_hbm.at[at], sems.at[k])
        copy.start()
        stores.append(copy)
    for k in range(head, steps):
        at = pl.ds(k * tile, tile)
        grad_buf[at, :] = gradient_tile(lhs_ref, inv_ref, centers_ref, rhs_ref, at)
        copy = pltpu.make_async_copy(grad_buf.at[at], grad_hbm.at[at], sems.at[k])
        copy.start()
        stores.append(copy)
        if k == head:
            x = emb_ref[...].astype(f32)
            inverse = lax.rsqrt(jnp.sum(x * x, axis=1, keepdims=True) + norm_eps)
            units = x * inverse
            total, slope, weight = (col_ref[:, at : at + 1] for at in range(3))
            picked = fin_ref[own:, :]
            grad = (fin_ref[:own, :] + weight * picked) / total - (logit_scale * slope) * picked
            emb_grad_buf[...] = inverse * (
                grad - units * jnp.sum(units * grad, axis=1, keepdims=True)
            )
            loss = jnp.broadcast_to(col_ref[:, 3:4], (own, lanes))
            diagonal = iota((own, lanes), 0) == iota((own, lanes), 1)
            loss_row = jnp.sum(jnp.where(diagonal, loss, 0.0), axis=0, keepdims=True)
            loss_buf[...] = loss_row[:, :own]
        if k == min(head + 1, steps - 1):
            for at, (src, dst) in enumerate(((emb_grad_buf, emb_grad_hbm), (loss_buf, loss_hbm))):
                copy = pltpu.make_async_copy(src, dst, sems.at[steps + at])
                copy.start()
                stores.append(copy)
    for copy in stores:
        copy.wait()


def per_device(n, embeddings, labels, centers):
    own, width = embeddings.shape
    count = centers.shape[0]
    batch = n * own
    wide = 2 * batch
    vmem = pl.BlockSpec(memory_space=pltpu.VMEM)
    dma = pltpu.SemaphoreType.DMA
    load = largest_tile(count, 512)
    hbm = pl.BlockSpec(memory_space=pltpu.HBM)
    tile = largest_tile(count, 256)
    fused = wide == lanes
    head = tile * min(4, count // tile - 1)
    cached, lhs, inv, rhs, fin, col, grad_head = pl.pallas_call(
        functools.partial(exchange_kernel, n, tile),
        out_shape=(
            jax.ShapeDtypeStruct((count, width), bf16),
            jax.ShapeDtypeStruct((count, 2 * wide if fused else wide), bf16),
            jax.ShapeDtypeStruct((count, lanes), f32),
            jax.ShapeDtypeStruct((4 * batch, width + lanes if fused else width), bf16),
            jax.ShapeDtypeStruct((2 * own, width), f32),
            jax.ShapeDtypeStruct((own, lanes), f32),
            jax.ShapeDtypeStruct((head, width), f32),
        ),
        in_specs=[hbm, hbm, hbm],
        out_specs=(vmem,) * 7,
        scratch_shapes=[
            pltpu.VMEM((count, width), bf16),
            pltpu.VMEM((own, width), bf16),
            pltpu.SMEM((own,), jnp.int32),
            pltpu.VMEM((n, own, width), bf16),
            pltpu.VMEM((n, 1, wide), jnp.int32),
            pltpu.VMEM((1, wide), f32),
            pltpu.VMEM((n - 1, 1, wide), f32),
            pltpu.VMEM((n, 2 * own, width), bf16),
            pltpu.VMEM((n - 1, 2 * own, width), bf16),
            pltpu.VMEM((batch, lanes), f32),
            dma((count // load,)),
            dma((2,)),
        ]
        + [dma((n - 1,))] * 8,
        compiler_params=pltpu.CompilerParams(
            collective_id=0, has_side_effects=True, vmem_limit_bytes=40 * 2**20
        ),
        name="exchange",
    )(*(pltpu.with_memory_space_constraint(v, pltpu.HBM) for v in (labels, embeddings, centers)))

    losses, emb_grad, center_grad = pl.pallas_call(
        functools.partial(gradient_kernel, tile),
        out_shape=(
            jax.ShapeDtypeStruct((1, own), f32),
            jax.ShapeDtypeStruct((own, width), f32),
            jax.ShapeDtypeStruct((count, width), f32),
        ),
        in_specs=[vmem] * 8,
        out_specs=(hbm,) * 3,
        scratch_shapes=[
            pltpu.VMEM((1, own), f32),
            pltpu.VMEM((own, width), f32),
            pltpu.VMEM((count, width), f32),
            dma((count // tile + 2,)),
        ],
        compiler_params=pltpu.CompilerParams(vmem_limit_bytes=32 * 2**20),
        name="gradient",
    )(lhs, inv, cached, rhs, embeddings, fin, col, grad_head)
    return losses.reshape(own), emb_grad, center_grad


def solution(mesh):
    in_specs = (P(("dp", "cls"), None), P(("dp", "cls")), P(("dp", "cls"), None))
    out_specs = (P(("dp", "cls")), P(("dp", "cls"), None), P(("dp", "cls"), None))
    return jax.shard_map(
        functools.partial(per_device, mesh.shape["cls"]),
        mesh=mesh,
        in_specs=in_specs,
        out_specs=out_specs,
        check_vma=False,
    )
```

```python
import functools
import math

import jax
import jax.numpy as jnp
from jax import lax
from jax.experimental import pallas as pl
from jax.experimental.pallas import tpu as pltpu
from jax.sharding import PartitionSpec as P

logit_scale = 64.0
margin_cosine = math.cos(0.5)
margin_sine = math.sin(0.5)
sine_soften = 0.04
norm_eps = 1e-06
lanes = 128
never = -1e30
log2_e = math.log2(math.e)
MESH = pl.DeviceIdType.MESH
f32 = jnp.float32
bf16 = jnp.bfloat16


def iota(shape, dim):
    return lax.broadcasted_iota(jnp.int32, shape, dim)


def largest_tile(count, limit):
    tile = limit
    while count % tile:
        tile //= 2
    return tile


def partner(me, n, k):
    if n & (n - 1):
        return lax.rem(me + k, n)
    bit, other = 1, me
    while bit < n:
        if k & bit:
            other = other + bit * (1 - 2 * lax.rem(me // bit, 2))
        bit *= 2
    return other


def gradient_tile(lhs_ref, inv_ref, centers_ref, rhs_ref, at):
    width = centers_ref.shape[1]
    repeat = width // lanes
    inverse = inv_ref[at, :]
    centers = centers_ref[at, :].astype(f32)
    lhs = lhs_ref[at, :]
    if rhs_ref.shape[1] > width:
        both = jnp.dot(lhs, rhs_ref[...], preferred_element_type=f32)
        grad = both[:, :width]
        back = both[:, width:] * (inverse * inverse)
    else:
        grad = jnp.dot(jnp.concatenate([lhs, lhs], axis=1), rhs_ref[...], preferred_element_type=f32)
        along = jnp.sum(centers * grad, axis=1, keepdims=True)
        back = along * (inverse * inverse * inverse)
    return (
        jnp.concatenate([inverse] * repeat, axis=1) * grad
        - jnp.concatenate([back] * repeat, axis=1) * centers
    )


def exchange_large(
    n,
    head_tile,
    labels_hbm,
    emb_hbm,
    centers_ref,
    cbuf,
    lhs_ref,
    inv_ref,
    rhs_ref,
    fin_ref,
    col_ref,
    head_ref,
    hat,
    emb_ref,
    labels_ref,
    xall,
    lall,
    stat,
    stat_in,
    part,
    part_in,
    colst,
    load_sem,
    small_sem,
    x_send,
    x_recv,
    l_send,
    l_recv,
    s_send,
    s_recv,
    p_send,
    p_recv,
):
    me = lax.axis_index("cls")
    own, width = emb_ref.shape
    count = cbuf.shape[0]
    batch = n * own
    wide = 2 * batch
    peers = [partner(me, n, k) for k in range(n - 1, 0, -1)]

    barrier = pltpu.get_barrier_semaphore()
    for peer in peers:
        pl.semaphore_signal(barrier, inc=1, device_id={"cls": peer}, device_id_type=MESH)

    small = [
        pltpu.make_async_copy(labels_hbm, labels_ref, small_sem.at[0]),
        pltpu.make_async_copy(emb_hbm, emb_ref, small_sem.at[1]),
    ]
    for copy in small:
        copy.start()
    load = largest_tile(count, 512)
    loads = []
    for k in range(count // load):
        copy = pltpu.make_async_copy(
            centers_ref.at[pl.ds(k * load, load)], cbuf.at[pl.ds(k * load, load)], load_sem.at[k]
        )
        copy.start()
        loads.append(copy)

    for copy in small:
        copy.wait()
    lane = iota((1, wide), 1)
    first = lane - me * own
    label_row = jnp.zeros((1, wide), jnp.int32)
    for i in range(own):
        label_row = jnp.where((first == i) | (first == batch + i), labels_ref[i], label_row)
    lall[me] = label_row
    x = emb_ref[...].astype(f32)
    xall[me] = (x * lax.rsqrt(jnp.sum(x * x, axis=1, keepdims=True) + norm_eps)).astype(bf16)

    def remote(src, dst, send, recv, peer):
        return pltpu.make_async_remote_copy(
            src_ref=src,
            dst_ref=dst,
            send_sem=send,
            recv_sem=recv,
            device_id={"cls": peer},
            device_id_type=MESH,
        )

    pl.semaphore_wait(barrier, n - 1)
    x_copies, l_copies = [], []
    for step, peer in enumerate(peers):
        copy = remote(xall.at[me], xall.at[me], x_send.at[step], x_recv.at[step], peer)
        copy.start()
        x_copies.append(copy)
        copy = remote(lall.at[me], lall.at[me], l_send.at[step], l_recv.at[step], peer)
        copy.start()
        l_copies.append(copy)

    sub = largest_tile(load, 64)
    for k in range(count // load):
        loads[k].wait()

        def norm(i, carry):
            at = pl.ds(pl.multiple_of(k * load + i * sub, sub), sub)
            c = cbuf[at, :].astype(f32)
            inverse = lax.rsqrt(jnp.sum(c * c, axis=1, keepdims=True) + norm_eps)
            inv_ref[at, :] = jnp.broadcast_to(inverse, (sub, lanes))
            hat[at, :] = (c * inverse).astype(bf16)
            return carry

        lax.fori_loop(0, load // sub, norm, 0, unroll=load // sub)

    for copy in x_copies + l_copies:
        copy.wait()

    x_hat = jnp.concatenate([xall[j] for j in range(n)], axis=0)
    x_both = jnp.concatenate([x_hat, x_hat], axis=0)
    label_row = lall[0]
    for j in range(1, n):
        label_row = label_row + lall[j]
    label_row = label_row - me * count
    bias = jnp.where(lane < batch, math.log2(logit_scale) - logit_scale * log2_e, never)
    one_hot_value = jnp.where(lane < batch, 0.0, 1.0)

    tile = largest_tile(count, 512 if wide <= 128 else 128)

    def score(k, sums):
        at = pl.ds(pl.multiple_of(k * tile, tile), tile)
        cosine = lax.dot_general(
            hat[at, :], x_both, (((1,), (1,)), ((), ())), preferred_element_type=f32
        )
        mask = iota((tile, wide), 0) == (label_row - k * tile)
        exps = jnp.exp2((logit_scale * log2_e) * cosine + bias)
        values = jnp.where(mask, one_hot_value, exps)
        products = values * cosine
        lhs_ref[at, :] = values.astype(bf16)
        counted = jnp.where(lane < batch, values, products)
        return sums + jnp.sum(counted.reshape(tile // 8, 8, wide), axis=0)

    sums = lax.fori_loop(0, count // tile, score, jnp.zeros((8, wide), f32))
    stat[...] = jnp.sum(sums, axis=0, keepdims=True)
    s_copies = []
    for step, peer in enumerate(peers):
        copy = remote(stat, stat_in.at[step], s_send.at[step], s_recv.at[step], peer)
        copy.start()
        s_copies.append(copy)

    summed = lax.dot_general(
        lhs_ref[...], hat[...], (((0,), (0,)), ((), ())), preferred_element_type=f32
    )
    for j in range(n):
        part[j] = jnp.concatenate(
            [summed[j * own : (j + 1) * own], summed[batch + j * own : batch + (j + 1) * own]],
            axis=0,
        ).astype(bf16)
    p_copies = []
    for step, peer in enumerate(peers):
        copy = remote(part.at[peer], part_in.at[step], p_send.at[step], p_recv.at[step], peer)
        copy.start()
        p_copies.append(copy)

    for copy in s_copies:
        copy.wait()
    sums = stat[...]
    for step in range(n - 1):
        sums = sums + stat_in[step]
    others = sums * (1.0 / logit_scale)
    target_cos = jnp.concatenate([sums[:, batch:], sums[:, :batch]], axis=1)
    target_sine = jnp.sqrt(1.0 + sine_soften - target_cos * target_cos)
    shifted = target_cos * margin_cosine - target_sine * margin_sine
    slope = margin_cosine + margin_sine * target_cos / target_sine
    label_exp = jnp.exp(logit_scale * shifted - logit_scale)
    totals = others + label_exp
    label_weight = (logit_scale * label_exp * slope).astype(bf16).astype(f32)
    losses = jnp.log(totals) + logit_scale - logit_scale * shifted
    stack_row = iota((lanes, wide), 0)
    stack = jnp.where(
        stack_row == 0,
        totals,
        jnp.where(stack_row == 1, slope, jnp.where(stack_row == 2, label_weight, losses)),
    )
    columns = stack.T
    colst[...] = columns[:batch]
    total_col = columns[:batch, 0:1]
    slope_col = columns[:batch, 1:2]
    weight_col = columns[:batch, 2:3]
    x_wide = x_hat.astype(f32)
    scaled = (x_wide / total_col).astype(bf16)
    label_term = weight_col * scaled.astype(f32) - (logit_scale * slope_col) * x_wide
    high = label_term.astype(bf16)
    low = (label_term - high.astype(f32)).astype(bf16)
    rhs_ref[...] = jnp.concatenate([scaled, high, jnp.zeros_like(high), low], axis=0)
    col_ref[...] = colst[pl.ds(pl.multiple_of(me * own, own), own), :]
    for k in range(head_ref.shape[0] // head_tile):
        at = pl.ds(k * head_tile, head_tile)
        head_ref[at, :] = gradient_tile(lhs_ref, inv_ref, cbuf, rhs_ref, at)

    for copy in p_copies:
        copy.wait()
    mine = part[me].astype(f32)
    for step in range(n - 1):
        mine = mine + part_in[step].astype(f32)
    fin_ref[...] = mine


def total_wait(ref, sem):
    pltpu.make_async_copy(ref, ref, sem).wait()


def swap_halves(row):
    half = row.shape[1] // 2
    return jnp.concatenate([row[:, half:], row[:, :half]], axis=1)


def margin_terms(sums):
    target_cos = swap_halves(sums)
    target_sine = jnp.sqrt(1.0 + sine_soften - target_cos * target_cos)
    shifted = target_cos * margin_cosine - target_sine * margin_sine
    slope = margin_cosine + margin_sine * target_cos / target_sine
    label_exp = jnp.exp(logit_scale * shifted - logit_scale)
    total = sums * (1.0 / logit_scale) + label_exp
    label_weight = (logit_scale * label_exp * slope).astype(bf16).astype(f32)
    return target_cos, shifted, slope, label_weight, total


def exchange_small(
    n,
    head_tile,
    labels_hbm,
    emb_hbm,
    centers_ref,
    cbuf,
    lhs_ref,
    inv_ref,
    rhs_ref,
    fin_ref,
    sums_ref,
    head_ref,
    hat,
    hat_t,
    w_t,
    emb_ref,
    labels_ref,
    xall,
    lall,
    stat,
    stat_in,
    part,
    part_in,
    load_sem,
    small_sem,
    send_sem,
    recv_sem,
):
    me = lax.axis_index("cls")
    own, width = emb_ref.shape
    count = cbuf.shape[0]
    batch = n * own
    half = lanes // 2
    peers = [partner(me, n, k) for k in range(n - 1, 0, -1)]

    barrier = pltpu.get_barrier_semaphore()
    for peer in peers:
        pl.semaphore_signal(barrier, inc=1, device_id={"cls": peer}, device_id_type=MESH)

    small = [
        pltpu.make_async_copy(labels_hbm, labels_ref, small_sem.at[0]),
        pltpu.make_async_copy(emb_hbm, emb_ref, small_sem.at[1]),
    ]
    for copy in small:
        copy.start()
    def send(src, dst, kind, peer):
        pltpu.make_async_remote_copy(
            src_ref=src,
            dst_ref=dst,
            send_sem=send_sem.at[kind],
            recv_sem=recv_sem.at[kind],
            device_id={"cls": peer},
            device_id_type=MESH,
        ).start()

    for copy in small:
        copy.wait()
    load = count // load_sem.shape[0]
    loads = []
    for k in range(count // load):
        at = pl.ds(k * load, load)
        copy = pltpu.make_async_copy(centers_ref.at[at], cbuf.at[at], load_sem.at[k])
        copy.start()
        loads.append(copy)

    label_rows = jnp.zeros((own, lanes), jnp.int32)
    for i in range(own):
        label_rows = jnp.where(iota((own, lanes), 0) == i, labels_ref[i], label_rows)
    lall[me] = label_rows
    x = emb_ref[...].astype(f32)
    xall[me] = (x * lax.rsqrt(jnp.sum(x * x, axis=1, keepdims=True) + norm_eps)).astype(bf16)

    pl.semaphore_wait(barrier, n - 1)
    for peer in peers:
        send(xall.at[me], xall.at[me], 0, peer)
        send(lall.at[me], lall.at[me], 1, peer)

    sub = largest_tile(load, 64)
    turn = largest_tile(load, 512)
    for k in range(count // load):
        loads[k].wait()
        for i in range(load // sub):
            at = pl.ds(k * load + i * sub, sub)
            c = cbuf[at, :].astype(f32)
            inverse = lax.rsqrt(jnp.sum(c * c, axis=1, keepdims=True) + norm_eps)
            inv_ref[at, :] = jnp.broadcast_to(inverse, (sub, lanes))
            hat[at, :] = (c * inverse).astype(bf16)
        for i in range(load // turn):
            at = pl.ds(k * load + i * turn, turn)
            hat_t[:, at] = hat[at, :].T

    total_wait(xall.at[pl.ds(0, n - 1)], recv_sem.at[0])
    total_wait(lall.at[pl.ds(0, n - 1)], recv_sem.at[1])

    x_hat = jnp.concatenate([xall[j] for j in range(n)], axis=0)
    label_col = jnp.concatenate([lall[j] for j in range(n)], axis=0) - me * count
    tile = largest_tile(count, 512)
    label_wide = jnp.concatenate([label_col] * (tile // lanes), axis=1)
    place = iota((batch, tile), 1)

    def lane_blocks(value):
        acc = value[:, :lanes]
        for i in range(1, value.shape[1] // lanes):
            acc = acc + value[:, i * lanes : (i + 1) * lanes]
        return acc

    others = jnp.zeros((batch, lanes), f32)
    picked = jnp.zeros((batch, lanes), f32)
    for k in range(count // tile):
        at = pl.ds(k * tile, tile)
        cosine = jnp.dot(x_hat, hat_t[:, at], preferred_element_type=f32)
        mask = place == label_wide - k * tile
        exps = jnp.exp2((logit_scale * log2_e) * cosine + (math.log2(logit_scale) - logit_scale * log2_e))
        values = jnp.where(mask, 0.0, exps)
        w_t[:batch, at] = values.astype(bf16)
        w_t[2 * batch : 3 * batch, at] = (values * cosine).astype(bf16)
        others = others + lane_blocks(values)
        picked = picked + lane_blocks(jnp.where(mask, cosine, 0.0))
    others = jnp.sum(others, axis=1, keepdims=True)
    picked = jnp.sum(picked, axis=1, keepdims=True)
    lane = iota((own, lanes), 1)
    mine = jnp.zeros((own, lanes), f32)
    for j in range(n):
        mine = jnp.where(lane == j, others[j * own : (j + 1) * own], mine)
        mine = jnp.where(lane == half + j, picked[j * own : (j + 1) * own], mine)
    stat[...] = mine
    for k, peer in enumerate(peers):
        send(stat, stat_in.at[k], 2, peer)

    for k in range(count // tile):
        at = pl.ds(k * tile, tile)
        one_hot = jnp.where(place == label_wide - k * tile, 1.0, 0.0).astype(bf16)
        w_t[batch : 2 * batch, at] = one_hot
        w_t[3 * batch :, at] = one_hot
    summed = jnp.dot(w_t[: 2 * batch, :], hat[...], preferred_element_type=f32)
    for j in range(n):
        part[j] = jnp.concatenate(
            [summed[j * own : (j + 1) * own], summed[batch + j * own : batch + (j + 1) * own]],
            axis=0,
        ).astype(bf16)
    for k, peer in enumerate(peers):
        send(part.at[peer], part_in.at[k], 3, peer)

    for k in range(count // tile):
        at = pl.ds(k * tile, tile)
        lhs_ref[at, :] = w_t[:, at].T

    total_wait(stat_in, recv_sem.at[2])
    sums = stat[...]
    for k in range(n - 1):
        sums = sums + stat_in[k]
    sums_ref[...] = sums
    target_cos, _, slope, label_weight, total = margin_terms(sums)

    def column(value):
        return jnp.concatenate([value[:, j : j + 1] for j in range(n)], axis=0)

    inverse = 1.0 / total
    pull = logit_scale * slope
    dot = (label_weight * inverse - pull) * target_cos
    inverse_col, pull_col, weight_col, dot_col = (
        column(v) for v in (inverse, pull, label_weight, dot)
    )
    x_wide = x_hat.astype(f32)
    scaled = (x_wide * inverse_col).astype(bf16)
    label_term = weight_col * scaled.astype(f32) - pull_col * x_wide
    high = label_term.astype(bf16)
    low = (label_term - high.astype(f32)).astype(bf16)
    dot_high = dot_col.astype(bf16)
    dot_low = (dot_col - dot_high.astype(f32)).astype(bf16)
    rhs_ref[:, :width] = jnp.concatenate([scaled, high, jnp.zeros_like(high), low], axis=0)
    rhs_ref[:, width:] = jnp.concatenate(
        [
            jnp.broadcast_to(v, (batch, lanes))
            for v in (jnp.zeros_like(dot_high), dot_high, inverse_col.astype(bf16), dot_low)
        ],
        axis=0,
    )
    for k in range(head_ref.shape[0] // head_tile):
        at = pl.ds(k * head_tile, head_tile)
        head_ref[at, :] = gradient_tile(lhs_ref, inv_ref, cbuf, rhs_ref, at)

    total_wait(part_in, recv_sem.at[3])
    mine = part[me].astype(f32)
    for k in range(n - 1):
        mine = mine + part_in[k].astype(f32)
    fin_ref[...] = mine
    total_wait(xall.at[pl.ds(0, n - 1)], send_sem.at[0])
    total_wait(lall.at[pl.ds(0, n - 1)], send_sem.at[1])
    total_wait(stat_in, send_sem.at[2])
    total_wait(part_in, send_sem.at[3])


def gradient_kernel(
    tile,
    lhs_ref,
    inv_ref,
    centers_ref,
    rhs_ref,
    emb_ref,
    fin_ref,
    col_ref,
    head_ref,
    loss_hbm,
    emb_grad_hbm,
    grad_hbm,
    loss_buf,
    emb_grad_buf,
    grad_buf,
    sems,
):
    own, width = emb_ref.shape
    count = lhs_ref.shape[0]
    fused = rhs_ref.shape[1] > width
    steps = count // tile
    head = head_ref.shape[0] // tile
    for k in range(head):
        at = pl.ds(k * tile, tile)
        pltpu.make_async_copy(head_ref.at[at], grad_hbm.at[at], sems.at[0]).start()
    for k in range(head, steps):
        at = pl.ds(k * tile, tile)
        grad_buf[at, :] = gradient_tile(lhs_ref, inv_ref, centers_ref, rhs_ref, at)
        pltpu.make_async_copy(grad_buf.at[at], grad_hbm.at[at], sems.at[0]).start()
        if k == head:
            x = emb_ref[...].astype(f32)
            inverse = lax.rsqrt(jnp.sum(x * x, axis=1, keepdims=True) + norm_eps)
            units = x * inverse
            if fused:
                here = iota((own, lanes), 1) == lax.axis_index("cls")
                _, shifted, slope, weight, total = (
                    jnp.sum(jnp.where(here, v, 0.0), axis=1, keepdims=True)
                    for v in margin_terms(col_ref[...])
                )
                loss = jnp.log(total) + logit_scale - logit_scale * shifted
            else:
                total, slope, weight, loss = (col_ref[:, at : at + 1] for at in range(4))
            picked = fin_ref[own:, :]
            grad = (fin_ref[:own, :] + weight * picked) / total - (logit_scale * slope) * picked
            emb_grad_buf[...] = inverse * (
                grad - units * jnp.sum(units * grad, axis=1, keepdims=True)
            )
            diagonal = iota((own, lanes), 0) == iota((own, lanes), 1)
            loss_row = jnp.sum(jnp.where(diagonal, jnp.broadcast_to(loss, (own, lanes)), 0.0), axis=0, keepdims=True)
            loss_buf[...] = loss_row[:, :own]
        if k == min(head + 1, steps - 1):
            pltpu.make_async_copy(emb_grad_buf, emb_grad_hbm, sems.at[1]).start()
            pltpu.make_async_copy(loss_buf, loss_hbm, sems.at[2]).start()
    total_wait(grad_hbm, sems.at[0])
    total_wait(emb_grad_hbm, sems.at[1])
    total_wait(loss_hbm, sems.at[2])


def per_device(n, embeddings, labels, centers):
    own, width = embeddings.shape
    count = centers.shape[0]
    batch = n * own
    wide = 2 * batch
    vmem = pl.BlockSpec(memory_space=pltpu.VMEM)
    dma = pltpu.SemaphoreType.DMA
    load = largest_tile(count, 512)
    hbm = pl.BlockSpec(memory_space=pltpu.HBM)
    tile = largest_tile(count, 256)
    fused = wide == lanes
    head = tile * min(1, count // tile - 1)
    if fused:
        kernel = exchange_small
        scratch = [
            pltpu.VMEM((count, width), bf16),
            pltpu.VMEM((width, count), bf16),
            pltpu.VMEM((4 * batch, count), bf16),
            pltpu.VMEM((own, width), bf16),
            pltpu.SMEM((own,), jnp.int32),
            pltpu.VMEM((n, own, width), bf16),
            pltpu.VMEM((n, own, lanes), jnp.int32),
            pltpu.VMEM((own, lanes), f32),
            pltpu.VMEM((n - 1, own, lanes), f32),
            pltpu.VMEM((n, 2 * own, width), bf16),
            pltpu.VMEM((n - 1, 2 * own, width), bf16),
            dma((count // largest_tile(count, 1024),)),
            dma((2,)),
            dma((4,)),
            dma((4,)),
        ]
    else:
        kernel = exchange_large
        scratch = [
            pltpu.VMEM((count, width), bf16),
            pltpu.VMEM((own, width), bf16),
            pltpu.SMEM((own,), jnp.int32),
            pltpu.VMEM((n, own, width), bf16),
            pltpu.VMEM((n, 1, wide), jnp.int32),
            pltpu.VMEM((1, wide), f32),
            pltpu.VMEM((n - 1, 1, wide), f32),
            pltpu.VMEM((n, 2 * own, width), bf16),
            pltpu.VMEM((n - 1, 2 * own, width), bf16),
            pltpu.VMEM((batch, lanes), f32),
            dma((count // load,)),
            dma((2,)),
        ] + [dma((n - 1,))] * 8
    cached, lhs, inv, rhs, fin, col, grad_head = pl.pallas_call(
        functools.partial(kernel, n, tile),
        out_shape=(
            jax.ShapeDtypeStruct((count, width), bf16),
            jax.ShapeDtypeStruct((count, 4 * batch if fused else wide), bf16),
            jax.ShapeDtypeStruct((count, lanes), f32),
            jax.ShapeDtypeStruct((4 * batch, width + lanes if fused else width), bf16),
            jax.ShapeDtypeStruct((2 * own, width), f32),
            jax.ShapeDtypeStruct((own, lanes), f32),
            jax.ShapeDtypeStruct((head, width), f32),
        ),
        in_specs=[hbm, hbm, hbm],
        out_specs=(vmem,) * 7,
        scratch_shapes=scratch,
        compiler_params=pltpu.CompilerParams(
            collective_id=0, has_side_effects=True, vmem_limit_bytes=40 * 2**20
        ),
        name="exchange",
    )(*(pltpu.with_memory_space_constraint(v, pltpu.HBM) for v in (labels, embeddings, centers)))

    losses, emb_grad, center_grad = pl.pallas_call(
        functools.partial(gradient_kernel, tile),
        out_shape=(
            jax.ShapeDtypeStruct((1, own), f32),
            jax.ShapeDtypeStruct((own, width), f32),
            jax.ShapeDtypeStruct((count, width), f32),
        ),
        in_specs=[vmem] * 8,
        out_specs=(hbm,) * 3,
        scratch_shapes=[
            pltpu.VMEM((1, own), f32),
            pltpu.VMEM((own, width), f32),
            pltpu.VMEM((count, width), f32),
            dma((3,)),
        ],
        compiler_params=pltpu.CompilerParams(vmem_limit_bytes=32 * 2**20),
        name="gradient",
    )(lhs, inv, cached, rhs, embeddings, fin, col, grad_head)
    return losses.reshape(own), emb_grad, center_grad


def solution(mesh):
    in_specs = (P(("dp", "cls"), None), P(("dp", "cls")), P(("dp", "cls"), None))
    out_specs = (P(("dp", "cls")), P(("dp", "cls"), None), P(("dp", "cls"), None))
    return jax.shard_map(
        functools.partial(per_device, mesh.shape["cls"]),
        mesh=mesh,
        in_specs=in_specs,
        out_specs=out_specs,
        check_vma=False,
    )
```

```python
import functools
import math

import jax
import jax.numpy as jnp
from jax import lax
from jax.experimental import pallas as pl
from jax.experimental.pallas import tpu as pltpu
from jax.sharding import PartitionSpec as P

logit_scale = 64.0
margin_cosine = math.cos(0.5)
margin_sine = math.sin(0.5)
sine_soften = 0.04
norm_eps = 1e-06
lanes = 128
never = -1e30
log2_e = math.log2(math.e)
MESH = pl.DeviceIdType.MESH
f32 = jnp.float32
bf16 = jnp.bfloat16


def iota(shape, dim):
    return lax.broadcasted_iota(jnp.int32, shape, dim)


def largest_tile(count, limit):
    tile = limit
    while count % tile:
        tile //= 2
    return tile


def partner(me, n, k):
    if n & (n - 1):
        return lax.rem(me + k, n)
    bit, other = 1, me
    while bit < n:
        if k & bit:
            other = other + bit * (1 - 2 * lax.rem(me // bit, 2))
        bit *= 2
    return other


def gradient_tile(lhs_ref, inv_ref, centers_ref, rhs_ref, at):
    width = centers_ref.shape[1]
    repeat = width // lanes
    inverse = inv_ref[at, :]
    centers = centers_ref[at, :].astype(f32)
    lhs = lhs_ref[at, :]
    if rhs_ref.shape[1] > width:
        both = jnp.dot(lhs, rhs_ref[...], preferred_element_type=f32)
        grad = both[:, :width]
        back = both[:, width:] * (inverse * inverse)
    else:
        grad = jnp.dot(jnp.concatenate([lhs, lhs], axis=1), rhs_ref[...], preferred_element_type=f32)
        along = jnp.sum(centers * grad, axis=1, keepdims=True)
        back = along * (inverse * inverse * inverse)
    return (
        jnp.concatenate([inverse] * repeat, axis=1) * grad
        - jnp.concatenate([back] * repeat, axis=1) * centers
    )


def exchange_large(
    n,
    head_tile,
    labels_hbm,
    emb_hbm,
    centers_ref,
    cbuf,
    lhs_ref,
    inv_ref,
    rhs_ref,
    fin_ref,
    col_ref,
    head_ref,
    hat,
    emb_ref,
    labels_ref,
    xall,
    lall,
    stat,
    stat_in,
    part,
    part_in,
    colst,
    load_sem,
    small_sem,
    x_send,
    x_recv,
    l_send,
    l_recv,
    s_send,
    s_recv,
    p_send,
    p_recv,
):
    me = lax.axis_index("cls")
    own, width = emb_ref.shape
    count = cbuf.shape[0]
    batch = n * own
    wide = 2 * batch
    peers = [partner(me, n, k) for k in range(n - 1, 0, -1)]

    barrier = pltpu.get_barrier_semaphore()
    for peer in peers:
        pl.semaphore_signal(barrier, inc=1, device_id={"cls": peer}, device_id_type=MESH)

    small = [
        pltpu.make_async_copy(labels_hbm, labels_ref, small_sem.at[0]),
        pltpu.make_async_copy(emb_hbm, emb_ref, small_sem.at[1]),
    ]
    for copy in small:
        copy.start()
    load = largest_tile(count, 512)
    loads = []
    for k in range(count // load):
        copy = pltpu.make_async_copy(
            centers_ref.at[pl.ds(k * load, load)], cbuf.at[pl.ds(k * load, load)], load_sem.at[k]
        )
        copy.start()
        loads.append(copy)

    for copy in small:
        copy.wait()
    lane = iota((1, wide), 1)
    first = lane - me * own
    label_row = jnp.zeros((1, wide), jnp.int32)
    for i in range(own):
        label_row = jnp.where((first == i) | (first == batch + i), labels_ref[i], label_row)
    lall[me] = label_row
    x = emb_ref[...].astype(f32)
    xall[me] = (x * lax.rsqrt(jnp.sum(x * x, axis=1, keepdims=True) + norm_eps)).astype(bf16)

    def remote(src, dst, send, recv, peer):
        return pltpu.make_async_remote_copy(
            src_ref=src,
            dst_ref=dst,
            send_sem=send,
            recv_sem=recv,
            device_id={"cls": peer},
            device_id_type=MESH,
        )

    pl.semaphore_wait(barrier, n - 1)
    x_copies, l_copies = [], []
    for step, peer in enumerate(peers):
        copy = remote(xall.at[me], xall.at[me], x_send.at[step], x_recv.at[step], peer)
        copy.start()
        x_copies.append(copy)
        copy = remote(lall.at[me], lall.at[me], l_send.at[step], l_recv.at[step], peer)
        copy.start()
        l_copies.append(copy)

    sub = largest_tile(load, 64)
    for k in range(count // load):
        loads[k].wait()

        def norm(i, carry):
            at = pl.ds(pl.multiple_of(k * load + i * sub, sub), sub)
            c = cbuf[at, :].astype(f32)
            inverse = lax.rsqrt(jnp.sum(c * c, axis=1, keepdims=True) + norm_eps)
            inv_ref[at, :] = jnp.broadcast_to(inverse, (sub, lanes))
            hat[at, :] = (c * inverse).astype(bf16)
            return carry

        lax.fori_loop(0, load // sub, norm, 0, unroll=load // sub)

    for copy in x_copies + l_copies:
        copy.wait()

    x_hat = jnp.concatenate([xall[j] for j in range(n)], axis=0)
    x_both = jnp.concatenate([x_hat, x_hat], axis=0)
    label_row = lall[0]
    for j in range(1, n):
        label_row = label_row + lall[j]
    label_row = label_row - me * count
    bias = jnp.where(lane < batch, math.log2(logit_scale) - logit_scale * log2_e, never)
    one_hot_value = jnp.where(lane < batch, 0.0, 1.0)

    tile = largest_tile(count, 512 if wide <= 128 else 128)

    def score(k, sums):
        at = pl.ds(pl.multiple_of(k * tile, tile), tile)
        cosine = lax.dot_general(
            hat[at, :], x_both, (((1,), (1,)), ((), ())), preferred_element_type=f32
        )
        mask = iota((tile, wide), 0) == (label_row - k * tile)
        exps = jnp.exp2((logit_scale * log2_e) * cosine + bias)
        values = jnp.where(mask, one_hot_value, exps)
        products = values * cosine
        lhs_ref[at, :] = values.astype(bf16)
        counted = jnp.where(lane < batch, values, products)
        return sums + jnp.sum(counted.reshape(tile // 8, 8, wide), axis=0)

    sums = lax.fori_loop(0, count // tile, score, jnp.zeros((8, wide), f32))
    stat[...] = jnp.sum(sums, axis=0, keepdims=True)
    s_copies = []
    for step, peer in enumerate(peers):
        copy = remote(stat, stat_in.at[step], s_send.at[step], s_recv.at[step], peer)
        copy.start()
        s_copies.append(copy)

    summed = lax.dot_general(
        lhs_ref[...], hat[...], (((0,), (0,)), ((), ())), preferred_element_type=f32
    )
    for j in range(n):
        part[j] = jnp.concatenate(
            [summed[j * own : (j + 1) * own], summed[batch + j * own : batch + (j + 1) * own]],
            axis=0,
        ).astype(bf16)
    p_copies = []
    for step, peer in enumerate(peers):
        copy = remote(part.at[peer], part_in.at[step], p_send.at[step], p_recv.at[step], peer)
        copy.start()
        p_copies.append(copy)

    for copy in s_copies:
        copy.wait()
    sums = stat[...]
    for step in range(n - 1):
        sums = sums + stat_in[step]
    others = sums * (1.0 / logit_scale)
    target_cos = jnp.concatenate([sums[:, batch:], sums[:, :batch]], axis=1)
    target_sine = jnp.sqrt(1.0 + sine_soften - target_cos * target_cos)
    shifted = target_cos * margin_cosine - target_sine * margin_sine
    slope = margin_cosine + margin_sine * target_cos / target_sine
    label_exp = jnp.exp(logit_scale * shifted - logit_scale)
    totals = others + label_exp
    label_weight = (logit_scale * label_exp * slope).astype(bf16).astype(f32)
    losses = jnp.log(totals) + logit_scale - logit_scale * shifted
    stack_row = iota((lanes, wide), 0)
    stack = jnp.where(
        stack_row == 0,
        totals,
        jnp.where(stack_row == 1, slope, jnp.where(stack_row == 2, label_weight, losses)),
    )
    columns = stack.T
    colst[...] = columns[:batch]
    total_col = columns[:batch, 0:1]
    slope_col = columns[:batch, 1:2]
    weight_col = columns[:batch, 2:3]
    x_wide = x_hat.astype(f32)
    scaled = (x_wide / total_col).astype(bf16)
    label_term = weight_col * scaled.astype(f32) - (logit_scale * slope_col) * x_wide
    high = label_term.astype(bf16)
    low = (label_term - high.astype(f32)).astype(bf16)
    rhs_ref[...] = jnp.concatenate([scaled, high, jnp.zeros_like(high), low], axis=0)
    col_ref[...] = colst[pl.ds(pl.multiple_of(me * own, own), own), :]
    for k in range(head_ref.shape[0] // head_tile):
        at = pl.ds(k * head_tile, head_tile)
        head_ref[at, :] = gradient_tile(lhs_ref, inv_ref, cbuf, rhs_ref, at)

    for copy in p_copies:
        copy.wait()
    mine = part[me].astype(f32)
    for step in range(n - 1):
        mine = mine + part_in[step].astype(f32)
    fin_ref[...] = mine


def total_wait(ref, sem):
    pltpu.make_async_copy(ref, ref, sem).wait()


def margin_terms(target_cos):
    target_sine = jnp.sqrt(1.0 + sine_soften - target_cos * target_cos)
    shifted = target_cos * margin_cosine - target_sine * margin_sine
    slope = margin_cosine + margin_sine * target_cos / target_sine
    label_exp = jnp.exp(logit_scale * shifted)
    label_weight = (label_exp * slope).astype(bf16).astype(f32)
    return shifted, slope, label_exp, label_weight


def exchange_small(
    n,
    head_tile,
    labels_hbm,
    emb_hbm,
    centers_ref,
    cbuf,
    lhs_ref,
    inv_ref,
    rhs_ref,
    fin_ref,
    sums_ref,
    head_ref,
    hat,
    hat_t,
    w_t,
    emb_ref,
    labels_ref,
    xall,
    lall,
    stat,
    stat_in,
    part,
    part_in,
    early_sums,
    load_sem,
    small_sem,
    send_sem,
    recv_sem,
):
    me = lax.axis_index("cls")
    own, width = emb_ref.shape
    count = cbuf.shape[0]
    batch = n * own
    half = lanes // 2
    peers = [partner(me, n, k) for k in range(n - 1, 0, -1)]

    barrier = pltpu.get_barrier_semaphore()
    for peer in peers:
        pl.semaphore_signal(barrier, inc=1, device_id={"cls": peer}, device_id_type=MESH)

    small = [
        pltpu.make_async_copy(labels_hbm, labels_ref, small_sem.at[0]),
        pltpu.make_async_copy(emb_hbm, emb_ref, small_sem.at[1]),
    ]
    for copy in small:
        copy.start()
    def send(src, dst, kind, peer):
        pltpu.make_async_remote_copy(
            src_ref=src,
            dst_ref=dst,
            send_sem=send_sem.at[kind],
            recv_sem=recv_sem.at[kind],
            device_id={"cls": peer},
            device_id_type=MESH,
        ).start()

    for copy in small:
        copy.wait()
    load = count // load_sem.shape[0]
    loads = []
    for k in range(count // load):
        at = pl.ds(k * load, load)
        copy = pltpu.make_async_copy(centers_ref.at[at], cbuf.at[at], load_sem.at[k])
        copy.start()
        loads.append(copy)

    lane = iota((own, lanes), 1)
    label_row = jnp.zeros((1, lanes), jnp.int32)
    for i in range(own):
        label_row = jnp.where(lane[:1] == i, labels_ref[i], label_row)
    lall[me] = label_row.astype(f32)
    x = emb_ref[...].astype(f32)
    xall[me] = (x * lax.rsqrt(jnp.sum(x * x, axis=1, keepdims=True) + norm_eps)).astype(bf16)

    pl.semaphore_wait(barrier, n - 1)
    for peer in peers:
        send(lall.at[me], lall.at[me], 3, peer)
        send(xall.at[me], xall.at[me], 0, peer)

    sub = largest_tile(load, 64)
    turn = largest_tile(load, 512)
    for k in range(count // load):
        loads[k].wait()
        for i in range(load // sub):
            at = pl.ds(k * load + i * sub, sub)
            c = cbuf[at, :].astype(f32)
            inverse = lax.rsqrt(jnp.sum(c * c, axis=1, keepdims=True) + norm_eps)
            inv_ref[at, :] = jnp.broadcast_to(inverse, (sub, lanes))
            hat[at, :] = (c * inverse).astype(bf16)
        for i in range(load // turn):
            at = pl.ds(k * load + i * turn, turn)
            hat_t[:, at] = hat[at, :].T

    total_wait(lall.at[pl.ds(0, n - 1)], recv_sem.at[3])
    total_wait(xall.at[pl.ds(0, n - 1)], recv_sem.at[0])

    x_hat = jnp.concatenate([xall[j] for j in range(n)], axis=0)
    diagonal = lane == iota((own, lanes), 0)
    labels = [jnp.sum(jnp.where(diagonal, lall[j], 0.0), axis=1, keepdims=True) for j in range(n)]
    label_col = jnp.concatenate(labels, axis=0).astype(jnp.int32) - me * count
    lane = iota((batch, lanes), 1)
    ahead = jnp.broadcast_to(label_col, (batch, lanes)) - lane
    tile = largest_tile(count, 256)
    blocks = range(tile // lanes)

    def one_hots(first, last):
        for k in range(first * tile, last * tile, lanes):
            at = pl.ds(k, lanes)
            one_hot = jnp.where(ahead == k, 1.0, 0.0).astype(bf16)
            w_t[batch : 2 * batch, at] = one_hot
            w_t[3 * batch :, at] = one_hot

    others = jnp.zeros((batch, lanes), f32)
    picked = jnp.zeros((batch, lanes), f32)
    for k in range(count // tile):
        wide_cosine = jnp.dot(
            x_hat, hat_t[:, k * tile : (k + 1) * tile], preferred_element_type=f32
        )
        for i in blocks:
            at = pl.ds(k * tile + i * lanes, lanes)
            cosine = wide_cosine[:, i * lanes : (i + 1) * lanes]
            mask = ahead == k * tile + i * lanes
            values = jnp.where(mask, 0.0, jnp.exp2((logit_scale * log2_e) * cosine))
            w_t[:batch, at] = values.astype(bf16)
            w_t[2 * batch : 3 * batch, at] = (values * cosine).astype(bf16)
            others = others + values
            picked = picked + jnp.where(mask, cosine, 0.0)
    early = count * 4 // 8
    one_hots(0, early // tile)
    early_sums[...] = jnp.dot(w_t[: 2 * batch, :early], hat[:early, :], preferred_element_type=f32)
    others = jnp.sum(others, axis=1, keepdims=True)
    picked = jnp.sum(picked, axis=1, keepdims=True)
    lane = lane[:own]
    mine = jnp.zeros((own, lanes), f32)
    for j in range(n):
        mine = jnp.where(lane == j, others[j * own : (j + 1) * own], mine)
        mine = jnp.where(lane == half + j, picked[j * own : (j + 1) * own], mine)
    stat[...] = mine
    for k, peer in enumerate(peers):
        send(stat, stat_in.at[k], 1, peer)

    total_wait(xall.at[pl.ds(0, n - 1)], send_sem.at[0])
    total_wait(lall.at[pl.ds(0, n - 1)], send_sem.at[3])
    one_hots(early // tile, count // tile)
    summed = early_sums[...] + jnp.dot(
        w_t[: 2 * batch, early:], hat[early:, :], preferred_element_type=f32
    )
    for j in range(n):
        part[j] = jnp.concatenate(
            [summed[j * own : (j + 1) * own], summed[batch + j * own : batch + (j + 1) * own]],
            axis=0,
        ).astype(bf16)
    for k, peer in enumerate(peers):
        send(part.at[peer], part_in.at[k], 2, peer)

    for k in range(count // tile):
        at = pl.ds(k * tile, tile)
        lhs_ref[at, :] = w_t[:, at].T

    total_wait(stat_in, recv_sem.at[1])
    sums = stat[...]
    for k in range(n - 1):
        sums = sums + stat_in[k]
    sums_ref[...] = sums
    _, slope, label_exp, label_weight = margin_terms(sums)

    def column(value, first):
        return jnp.concatenate([value[:, first + j : first + j + 1] for j in range(n)], axis=0)

    others_col = column(sums, 0)
    exp_col, pull_col, weight_col, target_col = (
        column(v, half) for v in (label_exp, logit_scale * slope, label_weight, sums)
    )
    inverse_col = logit_scale / (others_col + exp_col)
    dot_col = (weight_col * inverse_col - pull_col) * target_col
    x_wide = x_hat.astype(f32)
    scaled = (x_wide * inverse_col).astype(bf16)
    label_term = weight_col * scaled.astype(f32) - pull_col * x_wide
    high = label_term.astype(bf16)
    low = (label_term - high.astype(f32)).astype(bf16)
    dot_high = dot_col.astype(bf16)
    dot_low = (dot_col - dot_high.astype(f32)).astype(bf16)
    rhs_ref[:, :width] = jnp.concatenate([scaled, high, jnp.zeros_like(high), low], axis=0)
    rhs_ref[:, width:] = jnp.concatenate(
        [
            jnp.broadcast_to(v, (batch, lanes))
            for v in (jnp.zeros_like(dot_high), dot_high, inverse_col.astype(bf16), dot_low)
        ],
        axis=0,
    )
    for k in range(head_ref.shape[0] // head_tile):
        at = pl.ds(k * head_tile, head_tile)
        head_ref[at, :] = gradient_tile(lhs_ref, inv_ref, cbuf, rhs_ref, at)

    total_wait(part_in, recv_sem.at[2])
    mine = part[me].astype(f32)
    for k in range(n - 1):
        mine = mine + part_in[k].astype(f32)
    fin_ref[...] = mine
    total_wait(stat_in, send_sem.at[1])
    total_wait(part_in, send_sem.at[2])


def gradient_kernel(
    tile,
    lhs_ref,
    inv_ref,
    centers_ref,
    rhs_ref,
    emb_ref,
    fin_ref,
    col_ref,
    head_ref,
    loss_hbm,
    emb_grad_hbm,
    grad_hbm,
    loss_buf,
    emb_grad_buf,
    grad_buf,
    sems,
):
    own, width = emb_ref.shape
    count = lhs_ref.shape[0]
    fused = rhs_ref.shape[1] > width
    steps = count // tile
    head = head_ref.shape[0] // tile
    for k in range(head):
        at = pl.ds(k * tile, tile)
        pltpu.make_async_copy(head_ref.at[at], grad_hbm.at[at], sems.at[0]).start()
    for k in range(head, steps):
        at = pl.ds(k * tile, tile)
        grad_buf[at, :] = gradient_tile(lhs_ref, inv_ref, centers_ref, rhs_ref, at)
        pltpu.make_async_copy(grad_buf.at[at], grad_hbm.at[at], sems.at[0]).start()
        if k == head:
            x = emb_ref[...].astype(f32)
            inverse = lax.rsqrt(jnp.sum(x * x, axis=1, keepdims=True) + norm_eps)
            units = x * inverse
            if fused:
                me = lax.axis_index("cls")
                lane = iota((own, lanes), 1)
                others, target_cos = (
                    jnp.sum(jnp.where(lane == at, col_ref[...], 0.0), axis=1, keepdims=True)
                    for at in (me, me + lanes // 2)
                )
                shifted, slope, label_exp, weight = margin_terms(target_cos)
                total = others + label_exp
                loss = jnp.log(total) - logit_scale * shifted
                total = total * (1.0 / logit_scale)
            else:
                total, slope, weight, loss = (col_ref[:, at : at + 1] for at in range(4))
            picked = fin_ref[own:, :]
            grad = (fin_ref[:own, :] + weight * picked) / total - (logit_scale * slope) * picked
            emb_grad_buf[...] = inverse * (
                grad - units * jnp.sum(units * grad, axis=1, keepdims=True)
            )
            diagonal = iota((own, lanes), 0) == iota((own, lanes), 1)
            loss_row = jnp.sum(jnp.where(diagonal, jnp.broadcast_to(loss, (own, lanes)), 0.0), axis=0, keepdims=True)
            loss_buf[...] = loss_row[:, :own]
        if k == min(head + 1, steps - 1):
            pltpu.make_async_copy(emb_grad_buf, emb_grad_hbm, sems.at[1]).start()
            pltpu.make_async_copy(loss_buf, loss_hbm, sems.at[2]).start()
    total_wait(grad_hbm, sems.at[0])
    total_wait(emb_grad_hbm, sems.at[1])
    total_wait(loss_hbm, sems.at[2])


def per_device(n, embeddings, labels, centers):
    own, width = embeddings.shape
    count = centers.shape[0]
    batch = n * own
    wide = 2 * batch
    vmem = pl.BlockSpec(memory_space=pltpu.VMEM)
    dma = pltpu.SemaphoreType.DMA
    load = largest_tile(count, 512)
    hbm = pl.BlockSpec(memory_space=pltpu.HBM)
    tile = largest_tile(count, 256)
    fused = wide == lanes
    head = tile * min(2, count // tile - 1)
    if fused:
        kernel = exchange_small
        scratch = [
            pltpu.VMEM((count, width), bf16),
            pltpu.VMEM((width, count), bf16),
            pltpu.VMEM((4 * batch, count), bf16),
            pltpu.VMEM((own, width), bf16),
            pltpu.SMEM((own,), jnp.int32),
            pltpu.VMEM((n, own, width), bf16),
            pltpu.VMEM((n, 1, lanes), f32),
            pltpu.VMEM((own, lanes), f32),
            pltpu.VMEM((n - 1, own, lanes), f32),
            pltpu.VMEM((n, 2 * own, width), bf16),
            pltpu.VMEM((n - 1, 2 * own, width), bf16),
            pltpu.VMEM((2 * batch, width), f32),
            dma((4,)),
            dma((2,)),
            dma((4,)),
            dma((4,)),
        ]
    else:
        kernel = exchange_large
        scratch = [
            pltpu.VMEM((count, width), bf16),
            pltpu.VMEM((own, width), bf16),
            pltpu.SMEM((own,), jnp.int32),
            pltpu.VMEM((n, own, width), bf16),
            pltpu.VMEM((n, 1, wide), jnp.int32),
            pltpu.VMEM((1, wide), f32),
            pltpu.VMEM((n - 1, 1, wide), f32),
            pltpu.VMEM((n, 2 * own, width), bf16),
            pltpu.VMEM((n - 1, 2 * own, width), bf16),
            pltpu.VMEM((batch, lanes), f32),
            dma((count // load,)),
            dma((2,)),
        ] + [dma((n - 1,))] * 8
    cached, lhs, inv, rhs, fin, col, grad_head = pl.pallas_call(
        functools.partial(kernel, n, tile),
        out_shape=(
            jax.ShapeDtypeStruct((count, width), bf16),
            jax.ShapeDtypeStruct((count, 4 * batch if fused else wide), bf16),
            jax.ShapeDtypeStruct((count, lanes), f32),
            jax.ShapeDtypeStruct((4 * batch, width + lanes if fused else width), bf16),
            jax.ShapeDtypeStruct((2 * own, width), f32),
            jax.ShapeDtypeStruct((own, lanes), f32),
            jax.ShapeDtypeStruct((head, width), f32),
        ),
        in_specs=[hbm, hbm, hbm],
        out_specs=(vmem,) * 7,
        scratch_shapes=scratch,
        compiler_params=pltpu.CompilerParams(
            collective_id=0, has_side_effects=True, vmem_limit_bytes=40 * 2**20
        ),
        name="exchange",
    )(*(pltpu.with_memory_space_constraint(v, pltpu.HBM) for v in (labels, embeddings, centers)))

    losses, emb_grad, center_grad = pl.pallas_call(
        functools.partial(gradient_kernel, tile),
        out_shape=(
            jax.ShapeDtypeStruct((1, own), f32),
            jax.ShapeDtypeStruct((own, width), f32),
            jax.ShapeDtypeStruct((count, width), f32),
        ),
        in_specs=[vmem] * 8,
        out_specs=(hbm,) * 3,
        scratch_shapes=[
            pltpu.VMEM((1, own), f32),
            pltpu.VMEM((own, width), f32),
            pltpu.VMEM((count, width), f32),
            dma((3,)),
        ],
        compiler_params=pltpu.CompilerParams(vmem_limit_bytes=32 * 2**20),
        name="gradient",
    )(lhs, inv, cached, rhs, embeddings, fin, col, grad_head)
    return losses.reshape(own), emb_grad, center_grad


def solution(mesh):
    in_specs = (P(("dp", "cls"), None), P(("dp", "cls")), P(("dp", "cls"), None))
    out_specs = (P(("dp", "cls")), P(("dp", "cls"), None), P(("dp", "cls"), None))
    return jax.shard_map(
        functools.partial(per_device, mesh.shape["cls"]),
        mesh=mesh,
        in_specs=in_specs,
        out_specs=out_specs,
        check_vma=False,
    )
```

```python
import functools
import math

import jax
import jax.numpy as jnp
from jax import lax
from jax.experimental import pallas as pl
from jax.experimental.pallas import tpu as pltpu
from jax.sharding import PartitionSpec as P

logit_scale = 64.0
margin_cosine = math.cos(0.5)
margin_sine = math.sin(0.5)
sine_soften = 0.04
norm_eps = 1e-06
lanes = 128
never = -1e30
log2_e = math.log2(math.e)
MESH = pl.DeviceIdType.MESH
f32 = jnp.float32
bf16 = jnp.bfloat16


def iota(shape, dim):
    return lax.broadcasted_iota(jnp.int32, shape, dim)


def largest_tile(count, limit):
    tile = limit
    while count % tile:
        tile //= 2
    return tile


def partner(me, n, k):
    if n & (n - 1):
        return lax.rem(me + k, n)
    bit, other = 1, me
    while bit < n:
        if k & bit:
            other = other + bit * (1 - 2 * lax.rem(me // bit, 2))
        bit *= 2
    return other


def gradient_tile(lhs_ref, inv_ref, centers_ref, rhs_ref, at):
    width = centers_ref.shape[1]
    repeat = width // lanes
    inverse = inv_ref[at, :]
    centers = centers_ref[at, :].astype(f32)
    lhs = lhs_ref[at, :]
    if rhs_ref.shape[1] > width:
        both = jnp.dot(lhs, rhs_ref[...], preferred_element_type=f32)
        grad = both[:, :width]
        back = both[:, width:] * (inverse * inverse)
    else:
        grad = jnp.dot(jnp.concatenate([lhs, lhs], axis=1), rhs_ref[...], preferred_element_type=f32)
        along = jnp.sum(centers * grad, axis=1, keepdims=True)
        back = along * (inverse * inverse * inverse)
    return (
        jnp.concatenate([inverse] * repeat, axis=1) * grad
        - jnp.concatenate([back] * repeat, axis=1) * centers
    )


def exchange_large(
    n,
    head_tile,
    labels_hbm,
    emb_hbm,
    centers_ref,
    cbuf,
    lhs_ref,
    inv_ref,
    rhs_ref,
    fin_ref,
    col_ref,
    head_ref,
    hat,
    emb_ref,
    labels_ref,
    xall,
    lall,
    stat,
    stat_in,
    part,
    part_in,
    colst,
    load_sem,
    small_sem,
    x_send,
    x_recv,
    l_send,
    l_recv,
    s_send,
    s_recv,
    p_send,
    p_recv,
):
    me = lax.axis_index("cls")
    own, width = emb_ref.shape
    count = cbuf.shape[0]
    batch = n * own
    wide = 2 * batch
    peers = [partner(me, n, k) for k in range(n - 1, 0, -1)]

    barrier = pltpu.get_barrier_semaphore()
    for peer in peers:
        pl.semaphore_signal(barrier, inc=1, device_id={"cls": peer}, device_id_type=MESH)

    small = [
        pltpu.make_async_copy(labels_hbm, labels_ref, small_sem.at[0]),
        pltpu.make_async_copy(emb_hbm, emb_ref, small_sem.at[1]),
    ]
    for copy in small:
        copy.start()
    load = largest_tile(count, 512)
    loads = []
    for k in range(count // load):
        copy = pltpu.make_async_copy(
            centers_ref.at[pl.ds(k * load, load)], cbuf.at[pl.ds(k * load, load)], load_sem.at[k]
        )
        copy.start()
        loads.append(copy)

    for copy in small:
        copy.wait()
    lane = iota((1, wide), 1)
    first = lane - me * own
    label_row = jnp.zeros((1, wide), jnp.int32)
    for i in range(own):
        label_row = jnp.where((first == i) | (first == batch + i), labels_ref[i], label_row)
    lall[me] = label_row
    x = emb_ref[...].astype(f32)
    xall[me] = (x * lax.rsqrt(jnp.sum(x * x, axis=1, keepdims=True) + norm_eps)).astype(bf16)

    def remote(src, dst, send, recv, peer):
        return pltpu.make_async_remote_copy(
            src_ref=src,
            dst_ref=dst,
            send_sem=send,
            recv_sem=recv,
            device_id={"cls": peer},
            device_id_type=MESH,
        )

    pl.semaphore_wait(barrier, n - 1)
    x_copies, l_copies = [], []
    for step, peer in enumerate(peers):
        copy = remote(xall.at[me], xall.at[me], x_send.at[step], x_recv.at[step], peer)
        copy.start()
        x_copies.append(copy)
        copy = remote(lall.at[me], lall.at[me], l_send.at[step], l_recv.at[step], peer)
        copy.start()
        l_copies.append(copy)

    sub = largest_tile(load, 64)
    for k in range(count // load):
        loads[k].wait()

        def norm(i, carry):
            at = pl.ds(pl.multiple_of(k * load + i * sub, sub), sub)
            c = cbuf[at, :].astype(f32)
            inverse = lax.rsqrt(jnp.sum(c * c, axis=1, keepdims=True) + norm_eps)
            inv_ref[at, :] = jnp.broadcast_to(inverse, (sub, lanes))
            hat[at, :] = (c * inverse).astype(bf16)
            return carry

        lax.fori_loop(0, load // sub, norm, 0, unroll=load // sub)

    for copy in x_copies + l_copies:
        copy.wait()

    x_hat = jnp.concatenate([xall[j] for j in range(n)], axis=0)
    x_both = jnp.concatenate([x_hat, x_hat], axis=0)
    label_row = lall[0]
    for j in range(1, n):
        label_row = label_row + lall[j]
    label_row = label_row - me * count
    bias = jnp.where(lane < batch, math.log2(logit_scale) - logit_scale * log2_e, never)
    one_hot_value = jnp.where(lane < batch, 0.0, 1.0)

    tile = largest_tile(count, 512 if wide <= 128 else 128)

    def score(k, sums):
        at = pl.ds(pl.multiple_of(k * tile, tile), tile)
        cosine = lax.dot_general(
            hat[at, :], x_both, (((1,), (1,)), ((), ())), preferred_element_type=f32
        )
        mask = iota((tile, wide), 0) == (label_row - k * tile)
        exps = jnp.exp2((logit_scale * log2_e) * cosine + bias)
        values = jnp.where(mask, one_hot_value, exps)
        products = values * cosine
        lhs_ref[at, :] = values.astype(bf16)
        counted = jnp.where(lane < batch, values, products)
        return sums + jnp.sum(counted.reshape(tile // 8, 8, wide), axis=0)

    sums = lax.fori_loop(0, count // tile, score, jnp.zeros((8, wide), f32))
    stat[...] = jnp.sum(sums, axis=0, keepdims=True)
    s_copies = []
    for step, peer in enumerate(peers):
        copy = remote(stat, stat_in.at[step], s_send.at[step], s_recv.at[step], peer)
        copy.start()
        s_copies.append(copy)

    summed = lax.dot_general(
        lhs_ref[...], hat[...], (((0,), (0,)), ((), ())), preferred_element_type=f32
    )
    for j in range(n):
        part[j] = jnp.concatenate(
            [summed[j * own : (j + 1) * own], summed[batch + j * own : batch + (j + 1) * own]],
            axis=0,
        ).astype(bf16)
    p_copies = []
    for step, peer in enumerate(peers):
        copy = remote(part.at[peer], part_in.at[step], p_send.at[step], p_recv.at[step], peer)
        copy.start()
        p_copies.append(copy)

    for copy in s_copies:
        copy.wait()
    sums = stat[...]
    for step in range(n - 1):
        sums = sums + stat_in[step]
    others = sums * (1.0 / logit_scale)
    target_cos = jnp.concatenate([sums[:, batch:], sums[:, :batch]], axis=1)
    target_sine = jnp.sqrt(1.0 + sine_soften - target_cos * target_cos)
    shifted = target_cos * margin_cosine - target_sine * margin_sine
    slope = margin_cosine + margin_sine * target_cos / target_sine
    label_exp = jnp.exp(logit_scale * shifted - logit_scale)
    totals = others + label_exp
    label_weight = (logit_scale * label_exp * slope).astype(bf16).astype(f32)
    losses = jnp.log(totals) + logit_scale - logit_scale * shifted
    stack_row = iota((lanes, wide), 0)
    stack = jnp.where(
        stack_row == 0,
        totals,
        jnp.where(stack_row == 1, slope, jnp.where(stack_row == 2, label_weight, losses)),
    )
    columns = stack.T
    colst[...] = columns[:batch]
    total_col = columns[:batch, 0:1]
    slope_col = columns[:batch, 1:2]
    weight_col = columns[:batch, 2:3]
    x_wide = x_hat.astype(f32)
    scaled = (x_wide / total_col).astype(bf16)
    label_term = weight_col * scaled.astype(f32) - (logit_scale * slope_col) * x_wide
    high = label_term.astype(bf16)
    low = (label_term - high.astype(f32)).astype(bf16)
    rhs_ref[...] = jnp.concatenate([scaled, high, jnp.zeros_like(high), low], axis=0)
    col_ref[...] = colst[pl.ds(pl.multiple_of(me * own, own), own), :]
    for k in range(head_ref.shape[0] // head_tile):
        at = pl.ds(k * head_tile, head_tile)
        head_ref[at, :] = gradient_tile(lhs_ref, inv_ref, cbuf, rhs_ref, at)

    for copy in p_copies:
        copy.wait()
    mine = part[me].astype(f32)
    for step in range(n - 1):
        mine = mine + part_in[step].astype(f32)
    fin_ref[...] = mine


def total_wait(ref, sem):
    pltpu.make_async_copy(ref, ref, sem).wait()


def margin_terms(target_cos):
    target_sine = jnp.sqrt(1.0 + sine_soften - target_cos * target_cos)
    shifted = target_cos * margin_cosine - target_sine * margin_sine
    slope = margin_cosine + margin_sine * target_cos / target_sine
    label_exp = jnp.exp(logit_scale * shifted)
    label_weight = (label_exp * slope).astype(bf16).astype(f32)
    return shifted, slope, label_exp, label_weight


def exchange_small(
    n,
    head_tile,
    labels_hbm,
    emb_hbm,
    centers_ref,
    cbuf,
    lhs_ref,
    inv_ref,
    rhs_ref,
    fin_ref,
    sums_ref,
    head_ref,
    hat,
    hat_t,
    w_t,
    emb_ref,
    labels_ref,
    xall,
    lall,
    stat,
    stat_in,
    part,
    part_in,
    early_sums,
    sent,
    load_sem,
    small_sem,
    send_sem,
    recv_sem,
):
    me = lax.axis_index("cls")
    own, width = emb_ref.shape
    count = cbuf.shape[0]
    batch = n * own
    half = lanes // 2
    peers = [partner(me, n, k) for k in range(n - 1, 0, -1)]

    barrier = pltpu.get_barrier_semaphore()
    for peer in peers:
        pl.semaphore_signal(barrier, inc=1, device_id={"cls": peer}, device_id_type=MESH)

    small = [
        pltpu.make_async_copy(labels_hbm, labels_ref, small_sem.at[0]),
        pltpu.make_async_copy(emb_hbm, emb_ref, small_sem.at[1]),
    ]
    for copy in small:
        copy.start()
    def send(src, dst, kind, peer):
        pltpu.make_async_remote_copy(
            src_ref=src,
            dst_ref=dst,
            send_sem=send_sem.at[min(kind, 1)],
            recv_sem=recv_sem.at[kind],
            device_id={"cls": peer},
            device_id_type=MESH,
        ).start()

    def send_in_order(piece, into, kind):
        for j in range(n - 1):
            peer = j + (j >= me).astype(jnp.int32)
            send(piece(peer), into.at[me - (me > peer).astype(jnp.int32)], kind, peer)

    for copy in small:
        copy.wait()
    load = count // load_sem.shape[0]
    loads = []
    for k in range(count // load):
        at = pl.ds(k * load, load)
        copy = pltpu.make_async_copy(centers_ref.at[at], cbuf.at[at], load_sem.at[k])
        copy.start()
        loads.append(copy)

    lane = iota((own, lanes), 1)
    label_row = jnp.zeros((1, lanes), jnp.int32)
    for i in range(own):
        label_row = jnp.where(lane[:1] == i, labels_ref[i], label_row)
    lall[me] = label_row.astype(f32)
    x = emb_ref[...].astype(f32)
    xall[me] = (x * lax.rsqrt(jnp.sum(x * x, axis=1, keepdims=True) + norm_eps)).astype(bf16)

    pl.semaphore_wait(barrier, n - 1)
    for peer in peers:
        send(lall.at[me], lall.at[me], 3, peer)
        send(xall.at[me], xall.at[me], 0, peer)

    sub = largest_tile(load, 64)
    turn = largest_tile(load, 512)
    for k in range(count // load):
        loads[k].wait()
        for i in range(load // sub):
            at = pl.ds(k * load + i * sub, sub)
            c = cbuf[at, :].astype(f32)
            inverse = lax.rsqrt(jnp.sum(c * c, axis=1, keepdims=True) + norm_eps)
            inv_ref[at, :] = jnp.broadcast_to(inverse, (sub, lanes))
            hat[at, :] = (c * inverse).astype(bf16)
        for i in range(load // turn):
            at = pl.ds(k * load + i * turn, turn)
            hat_t[:, at] = hat[at, :].T

    total_wait(lall.at[pl.ds(0, n - 1)], recv_sem.at[3])
    total_wait(xall.at[pl.ds(0, n - 1)], recv_sem.at[0])

    x_hat = jnp.concatenate([xall[j] for j in range(n)], axis=0)
    diagonal = lane == iota((own, lanes), 0)
    labels = [jnp.sum(jnp.where(diagonal, lall[j], 0.0), axis=1, keepdims=True) for j in range(n)]
    label_col = jnp.concatenate(labels, axis=0).astype(jnp.int32) - me * count
    lane = iota((batch, lanes), 1)
    ahead = jnp.broadcast_to(label_col, (batch, lanes)) - lane
    tile = largest_tile(count, 256)
    blocks = range(tile // lanes)

    def one_hots(first, last):
        for k in range(first * tile, last * tile, lanes):
            at = pl.ds(k, lanes)
            one_hot = jnp.where(ahead == k, 1.0, 0.0).astype(bf16)
            w_t[batch : 2 * batch, at] = one_hot
            w_t[3 * batch :, at] = one_hot

    others = jnp.zeros((batch, lanes), f32)
    picked = jnp.zeros((batch, lanes), f32)
    for k in range(count // tile):
        wide_cosine = jnp.dot(
            x_hat, hat_t[:, k * tile : (k + 1) * tile], preferred_element_type=f32
        )
        for i in blocks:
            at = pl.ds(k * tile + i * lanes, lanes)
            cosine = wide_cosine[:, i * lanes : (i + 1) * lanes]
            mask = ahead == k * tile + i * lanes
            values = jnp.where(mask, 0.0, jnp.exp2((logit_scale * log2_e) * cosine))
            w_t[:batch, at] = values.astype(bf16)
            w_t[2 * batch : 3 * batch, at] = (values * cosine).astype(bf16)
            others = others + values
            picked = picked + jnp.where(mask, cosine, 0.0)
    early = count * 3 // 8
    one_hots(0, early // tile)
    early_sums[...] = jnp.dot(w_t[: 2 * batch, :early], hat[:early, :], preferred_element_type=f32)
    others = jnp.sum(others, axis=1, keepdims=True)
    picked = jnp.sum(picked, axis=1, keepdims=True)
    lane = lane[:own]
    mine = jnp.zeros((own, lanes), f32)
    for j in range(n):
        mine = jnp.where(lane == j, others[j * own : (j + 1) * own], mine)
        mine = jnp.where(lane == half + j, picked[j * own : (j + 1) * own], mine)
    stat[...] = mine
    for k, peer in enumerate(peers):
        send(stat, stat_in.at[k], 1, peer)

    total_wait(xall.at[pl.ds(0, n - 1)], send_sem.at[0])
    one_hots(early // tile, count // tile)
    summed = early_sums[...] + jnp.dot(
        w_t[: 2 * batch, early:], hat[early:, :], preferred_element_type=f32
    )
    for j in range(n):
        part[j] = jnp.concatenate(
            [summed[j * own : (j + 1) * own], summed[batch + j * own : batch + (j + 1) * own]],
            axis=0,
        ).astype(bf16)
    send_in_order(lambda peer: part.at[peer], part_in, 2)

    for k in range(count // tile):
        at = pl.ds(k * tile, tile)
        lhs_ref[at, :] = w_t[:, at].T

    total_wait(stat_in, recv_sem.at[1])
    sums = stat[...]
    for k in range(n - 1):
        sums = sums + stat_in[k]
    sums_ref[...] = sums
    _, slope, label_exp, label_weight = margin_terms(sums)

    def column(value, first):
        return jnp.concatenate(
            [
                jnp.broadcast_to(value[:, first + j : first + j + 1], (own, lanes))
                for j in range(n)
            ],
            axis=0,
        )

    others_col = column(sums, 0)
    exp_col, pull_col, weight_col, target_col = (
        column(v, half) for v in (label_exp, logit_scale * slope, label_weight, sums)
    )
    inverse_col = logit_scale / (others_col + exp_col)
    dot_col = (weight_col * inverse_col - pull_col) * target_col
    x_wide = x_hat.astype(f32)
    inverse_wide, pull_wide, weight_wide = (
        jnp.concatenate([v] * (width // lanes), axis=1)
        for v in (inverse_col, pull_col, weight_col)
    )
    scaled = (x_wide * inverse_wide).astype(bf16)
    label_term = weight_wide * scaled.astype(f32) - pull_wide * x_wide
    high = label_term.astype(bf16)
    low = (label_term - high.astype(f32)).astype(bf16)
    dot_high = dot_col.astype(bf16)
    dot_low = (dot_col - dot_high.astype(f32)).astype(bf16)
    rhs_ref[:, :width] = jnp.concatenate([scaled, high, jnp.zeros_like(high), low], axis=0)
    rhs_ref[:, width:] = jnp.concatenate(
        [jnp.zeros_like(dot_high), dot_high, inverse_col.astype(bf16), dot_low], axis=0
    )
    for k in range(head_ref.shape[0] // head_tile):
        at = pl.ds(k * head_tile, head_tile)
        head_ref[at, :] = gradient_tile(lhs_ref, inv_ref, cbuf, rhs_ref, at)

    total_wait(part_in, recv_sem.at[2])
    mine = part[me].astype(f32)
    for k in range(n - 1):
        mine = mine + part_in[k].astype(f32)
    fin_ref[...] = mine
    total_wait(sent, send_sem.at[1])


def gradient_kernel(
    tile,
    lhs_ref,
    inv_ref,
    centers_ref,
    rhs_ref,
    emb_ref,
    fin_ref,
    col_ref,
    head_ref,
    loss_hbm,
    emb_grad_hbm,
    grad_hbm,
    loss_buf,
    emb_grad_buf,
    grad_buf,
    sems,
):
    own, width = emb_ref.shape
    count = lhs_ref.shape[0]
    fused = rhs_ref.shape[1] > width
    steps = count // tile
    head = head_ref.shape[0] // tile
    for k in range(head):
        at = pl.ds(k * tile, tile)
        pltpu.make_async_copy(head_ref.at[at], grad_hbm.at[at], sems.at[0]).start()
    for k in range(head, steps):
        at = pl.ds(k * tile, tile)
        grad_buf[at, :] = gradient_tile(lhs_ref, inv_ref, centers_ref, rhs_ref, at)
        pltpu.make_async_copy(grad_buf.at[at], grad_hbm.at[at], sems.at[0]).start()
        if k == head:
            x = emb_ref[...].astype(f32)
            inverse = lax.rsqrt(jnp.sum(x * x, axis=1, keepdims=True) + norm_eps)
            units = x * inverse
            if fused:
                me = lax.axis_index("cls")
                lane = iota((own, lanes), 1)
                others, target_cos = (
                    jnp.sum(jnp.where(lane == at, col_ref[...], 0.0), axis=1, keepdims=True)
                    for at in (me, me + lanes // 2)
                )
                shifted, slope, label_exp, weight = margin_terms(target_cos)
                total = others + label_exp
                loss = jnp.log(total) - logit_scale * shifted
                total = total * (1.0 / logit_scale)
            else:
                total, slope, weight, loss = (col_ref[:, at : at + 1] for at in range(4))
            picked = fin_ref[own:, :]
            grad = (fin_ref[:own, :] + weight * picked) / total - (logit_scale * slope) * picked
            emb_grad_buf[...] = inverse * (
                grad - units * jnp.sum(units * grad, axis=1, keepdims=True)
            )
            diagonal = iota((own, lanes), 0) == iota((own, lanes), 1)
            loss_row = jnp.sum(jnp.where(diagonal, jnp.broadcast_to(loss, (own, lanes)), 0.0), axis=0, keepdims=True)
            loss_buf[...] = loss_row[:, :own]
        if k == min(head + 1, steps - 1):
            pltpu.make_async_copy(emb_grad_buf, emb_grad_hbm, sems.at[1]).start()
            pltpu.make_async_copy(loss_buf, loss_hbm, sems.at[2]).start()
    total_wait(grad_hbm, sems.at[0])
    total_wait(emb_grad_hbm, sems.at[1])
    total_wait(loss_hbm, sems.at[2])


def per_device(n, embeddings, labels, centers):
    own, width = embeddings.shape
    count = centers.shape[0]
    batch = n * own
    wide = 2 * batch
    vmem = pl.BlockSpec(memory_space=pltpu.VMEM)
    dma = pltpu.SemaphoreType.DMA
    load = largest_tile(count, 512)
    hbm = pl.BlockSpec(memory_space=pltpu.HBM)
    tile = largest_tile(count, 256)
    fused = wide == lanes
    head = tile * min(2, count // tile - 1)
    if fused:
        kernel = exchange_small
        scratch = [
            pltpu.VMEM((count, width), bf16),
            pltpu.VMEM((width, count), bf16),
            pltpu.VMEM((4 * batch, count), bf16),
            pltpu.VMEM((own, width), bf16),
            pltpu.SMEM((own,), jnp.int32),
            pltpu.VMEM((n, own, width), bf16),
            pltpu.VMEM((n, 1, lanes), f32),
            pltpu.VMEM((own, lanes), f32),
            pltpu.VMEM((n - 1, own, lanes), f32),
            pltpu.VMEM((n, 2 * own, width), bf16),
            pltpu.VMEM((n - 1, 2 * own, width), bf16),
            pltpu.VMEM((2 * batch, width), f32),
            pltpu.VMEM(((n - 1) * (1 + own + own * width // lanes), 1, lanes), f32),
            dma((4,)),
            dma((2,)),
            dma((2,)),
            dma((4,)),
        ]
    else:
        kernel = exchange_large
        scratch = [
            pltpu.VMEM((count, width), bf16),
            pltpu.VMEM((own, width), bf16),
            pltpu.SMEM((own,), jnp.int32),
            pltpu.VMEM((n, own, width), bf16),
            pltpu.VMEM((n, 1, wide), jnp.int32),
            pltpu.VMEM((1, wide), f32),
            pltpu.VMEM((n - 1, 1, wide), f32),
            pltpu.VMEM((n, 2 * own, width), bf16),
            pltpu.VMEM((n - 1, 2 * own, width), bf16),
            pltpu.VMEM((batch, lanes), f32),
            dma((count // load,)),
            dma((2,)),
        ] + [dma((n - 1,))] * 8
    cached, lhs, inv, rhs, fin, col, grad_head = pl.pallas_call(
        functools.partial(kernel, n, tile),
        out_shape=(
            jax.ShapeDtypeStruct((count, width), bf16),
            jax.ShapeDtypeStruct((count, 4 * batch if fused else wide), bf16),
            jax.ShapeDtypeStruct((count, lanes), f32),
            jax.ShapeDtypeStruct((4 * batch, width + lanes if fused else width), bf16),
            jax.ShapeDtypeStruct((2 * own, width), f32),
            jax.ShapeDtypeStruct((own, lanes), f32),
            jax.ShapeDtypeStruct((head, width), f32),
        ),
        in_specs=[hbm, hbm, hbm],
        out_specs=(vmem,) * 7,
        scratch_shapes=scratch,
        compiler_params=pltpu.CompilerParams(
            collective_id=0, has_side_effects=True, vmem_limit_bytes=40 * 2**20
        ),
        name="exchange",
    )(*(pltpu.with_memory_space_constraint(v, pltpu.HBM) for v in (labels, embeddings, centers)))

    losses, emb_grad, center_grad = pl.pallas_call(
        functools.partial(gradient_kernel, tile),
        out_shape=(
            jax.ShapeDtypeStruct((1, own), f32),
            jax.ShapeDtypeStruct((own, width), f32),
            jax.ShapeDtypeStruct((count, width), f32),
        ),
        in_specs=[vmem] * 8,
        out_specs=(hbm,) * 3,
        scratch_shapes=[
            pltpu.VMEM((1, own), f32),
            pltpu.VMEM((own, width), f32),
            pltpu.VMEM((count, width), f32),
            dma((3,)),
        ],
        compiler_params=pltpu.CompilerParams(vmem_limit_bytes=32 * 2**20),
        name="gradient",
    )(lhs, inv, cached, rhs, embeddings, fin, col, grad_head)
    return losses.reshape(own), emb_grad, center_grad


def solution(mesh):
    in_specs = (P(("dp", "cls"), None), P(("dp", "cls")), P(("dp", "cls"), None))
    out_specs = (P(("dp", "cls")), P(("dp", "cls"), None), P(("dp", "cls"), None))
    return jax.shard_map(
        functools.partial(per_device, mesh.shape["cls"]),
        mesh=mesh,
        in_specs=in_specs,
        out_specs=out_specs,
        check_vma=False,
    )
```

```python
import functools
import math

import jax
import jax.numpy as jnp
from jax import lax
from jax.experimental import pallas as pl
from jax.experimental.pallas import tpu as pltpu
from jax.sharding import PartitionSpec as P

logit_scale = 64.0
margin_cosine = math.cos(0.5)
margin_sine = math.sin(0.5)
sine_soften = 0.04
norm_eps = 1e-06
lanes = 128
never = -1e30
log2_e = math.log2(math.e)
MESH = pl.DeviceIdType.MESH
f32 = jnp.float32
bf16 = jnp.bfloat16


def iota(shape, dim):
    return lax.broadcasted_iota(jnp.int32, shape, dim)


def largest_tile(count, limit):
    tile = limit
    while count % tile:
        tile //= 2
    return tile


def partner(me, n, k):
    if n & (n - 1):
        return lax.rem(me + k, n)
    bit, other = 1, me
    while bit < n:
        if k & bit:
            other = other + bit * (1 - 2 * lax.rem(me // bit, 2))
        bit *= 2
    return other


def gradient_tile(lhs_ref, inv_ref, centers_ref, rhs_ref, at):
    width = centers_ref.shape[1]
    repeat = width // lanes
    inverse = inv_ref[at, :]
    centers = centers_ref[at, :].astype(f32)
    lhs = lhs_ref[at, :]
    if rhs_ref.shape[1] > width:
        both = jnp.dot(lhs, rhs_ref[...], preferred_element_type=f32)
        grad = both[:, :width]
        back = both[:, width:] * (inverse * inverse)
    else:
        grad = jnp.dot(jnp.concatenate([lhs, lhs], axis=1), rhs_ref[...], preferred_element_type=f32)
        along = jnp.sum(centers * grad, axis=1, keepdims=True)
        back = along * (inverse * inverse * inverse)
    return (
        jnp.concatenate([inverse] * repeat, axis=1) * grad
        - jnp.concatenate([back] * repeat, axis=1) * centers
    )


def exchange_large(
    n,
    head_tile,
    labels_hbm,
    emb_hbm,
    centers_ref,
    cbuf,
    lhs_ref,
    inv_ref,
    rhs_ref,
    fin_ref,
    col_ref,
    head_ref,
    hat,
    emb_ref,
    labels_ref,
    xall,
    lall,
    stat,
    stat_in,
    part,
    part_in,
    colst,
    load_sem,
    small_sem,
    x_send,
    x_recv,
    l_send,
    l_recv,
    s_send,
    s_recv,
    p_send,
    p_recv,
):
    me = lax.axis_index("cls")
    own, width = emb_ref.shape
    count = cbuf.shape[0]
    batch = n * own
    wide = 2 * batch
    peers = [partner(me, n, k) for k in range(n - 1, 0, -1)]

    barrier = pltpu.get_barrier_semaphore()
    for peer in peers:
        pl.semaphore_signal(barrier, inc=1, device_id={"cls": peer}, device_id_type=MESH)

    small = [
        pltpu.make_async_copy(labels_hbm, labels_ref, small_sem.at[0]),
        pltpu.make_async_copy(emb_hbm, emb_ref, small_sem.at[1]),
    ]
    for copy in small:
        copy.start()
    load = largest_tile(count, 512)
    loads = []
    for k in range(count // load):
        copy = pltpu.make_async_copy(
            centers_ref.at[pl.ds(k * load, load)], cbuf.at[pl.ds(k * load, load)], load_sem.at[k]
        )
        copy.start()
        loads.append(copy)

    for copy in small:
        copy.wait()
    lane = iota((1, wide), 1)
    first = lane - me * own
    label_row = jnp.zeros((1, wide), jnp.int32)
    for i in range(own):
        label_row = jnp.where((first == i) | (first == batch + i), labels_ref[i], label_row)
    lall[me] = label_row
    x = emb_ref[...].astype(f32)
    xall[me] = (x * lax.rsqrt(jnp.sum(x * x, axis=1, keepdims=True) + norm_eps)).astype(bf16)

    def remote(src, dst, send, recv, peer):
        return pltpu.make_async_remote_copy(
            src_ref=src,
            dst_ref=dst,
            send_sem=send,
            recv_sem=recv,
            device_id={"cls": peer},
            device_id_type=MESH,
        )

    pl.semaphore_wait(barrier, n - 1)
    x_copies, l_copies = [], []
    for step, peer in enumerate(peers):
        copy = remote(xall.at[me], xall.at[me], x_send.at[step], x_recv.at[step], peer)
        copy.start()
        x_copies.append(copy)
        copy = remote(lall.at[me], lall.at[me], l_send.at[step], l_recv.at[step], peer)
        copy.start()
        l_copies.append(copy)

    sub = largest_tile(load, 64)
    for k in range(count // load):
        loads[k].wait()

        def norm(i, carry):
            at = pl.ds(pl.multiple_of(k * load + i * sub, sub), sub)
            c = cbuf[at, :].astype(f32)
            inverse = lax.rsqrt(jnp.sum(c * c, axis=1, keepdims=True) + norm_eps)
            inv_ref[at, :] = jnp.broadcast_to(inverse, (sub, lanes))
            hat[at, :] = (c * inverse).astype(bf16)
            return carry

        lax.fori_loop(0, load // sub, norm, 0, unroll=load // sub)

    for copy in x_copies + l_copies:
        copy.wait()

    x_hat = jnp.concatenate([xall[j] for j in range(n)], axis=0)
    x_both = jnp.concatenate([x_hat, x_hat], axis=0)
    label_row = lall[0]
    for j in range(1, n):
        label_row = label_row + lall[j]
    label_row = label_row - me * count
    bias = jnp.where(lane < batch, math.log2(logit_scale) - logit_scale * log2_e, never)
    one_hot_value = jnp.where(lane < batch, 0.0, 1.0)

    tile = largest_tile(count, 512 if wide <= 128 else 128)

    def score(k, sums):
        at = pl.ds(pl.multiple_of(k * tile, tile), tile)
        cosine = lax.dot_general(
            hat[at, :], x_both, (((1,), (1,)), ((), ())), preferred_element_type=f32
        )
        mask = iota((tile, wide), 0) == (label_row - k * tile)
        exps = jnp.exp2((logit_scale * log2_e) * cosine + bias)
        values = jnp.where(mask, one_hot_value, exps)
        products = values * cosine
        lhs_ref[at, :] = values.astype(bf16)
        counted = jnp.where(lane < batch, values, products)
        return sums + jnp.sum(counted.reshape(tile // 8, 8, wide), axis=0)

    sums = lax.fori_loop(0, count // tile, score, jnp.zeros((8, wide), f32))
    stat[...] = jnp.sum(sums, axis=0, keepdims=True)
    s_copies = []
    for step, peer in enumerate(peers):
        copy = remote(stat, stat_in.at[step], s_send.at[step], s_recv.at[step], peer)
        copy.start()
        s_copies.append(copy)

    summed = lax.dot_general(
        lhs_ref[...], hat[...], (((0,), (0,)), ((), ())), preferred_element_type=f32
    )
    for j in range(n):
        part[j] = jnp.concatenate(
            [summed[j * own : (j + 1) * own], summed[batch + j * own : batch + (j + 1) * own]],
            axis=0,
        ).astype(bf16)
    p_copies = []
    for step, peer in enumerate(peers):
        copy = remote(part.at[peer], part_in.at[step], p_send.at[step], p_recv.at[step], peer)
        copy.start()
        p_copies.append(copy)

    for copy in s_copies:
        copy.wait()
    sums = stat[...]
    for step in range(n - 1):
        sums = sums + stat_in[step]
    others = sums * (1.0 / logit_scale)
    target_cos = jnp.concatenate([sums[:, batch:], sums[:, :batch]], axis=1)
    target_sine = jnp.sqrt(1.0 + sine_soften - target_cos * target_cos)
    shifted = target_cos * margin_cosine - target_sine * margin_sine
    slope = margin_cosine + margin_sine * target_cos / target_sine
    label_exp = jnp.exp(logit_scale * shifted - logit_scale)
    totals = others + label_exp
    label_weight = (logit_scale * label_exp * slope).astype(bf16).astype(f32)
    losses = jnp.log(totals) + logit_scale - logit_scale * shifted
    stack_row = iota((lanes, wide), 0)
    stack = jnp.where(
        stack_row == 0,
        totals,
        jnp.where(stack_row == 1, slope, jnp.where(stack_row == 2, label_weight, losses)),
    )
    columns = stack.T
    colst[...] = columns[:batch]
    total_col = columns[:batch, 0:1]
    slope_col = columns[:batch, 1:2]
    weight_col = columns[:batch, 2:3]
    x_wide = x_hat.astype(f32)
    scaled = (x_wide / total_col).astype(bf16)
    label_term = weight_col * scaled.astype(f32) - (logit_scale * slope_col) * x_wide
    high = label_term.astype(bf16)
    low = (label_term - high.astype(f32)).astype(bf16)
    rhs_ref[...] = jnp.concatenate([scaled, high, jnp.zeros_like(high), low], axis=0)
    col_ref[...] = colst[pl.ds(pl.multiple_of(me * own, own), own), :]
    for k in range(head_ref.shape[0] // head_tile):
        at = pl.ds(k * head_tile, head_tile)
        head_ref[at, :] = gradient_tile(lhs_ref, inv_ref, cbuf, rhs_ref, at)

    for copy in p_copies:
        copy.wait()
    mine = part[me].astype(f32)
    for step in range(n - 1):
        mine = mine + part_in[step].astype(f32)
    fin_ref[...] = mine


def total_wait(ref, sem):
    pltpu.make_async_copy(ref, ref, sem).wait()


def margin_terms(target_cos):
    sine_squared = 1.0 + sine_soften - target_cos * target_cos
    sine_inverse = lax.rsqrt(sine_squared)
    shifted = target_cos * margin_cosine - sine_squared * sine_inverse * margin_sine
    slope = margin_cosine + margin_sine * target_cos * sine_inverse
    label_exp = jnp.exp(logit_scale * shifted)
    label_weight = (label_exp * slope).astype(bf16).astype(f32)
    return shifted, slope, label_exp, label_weight


def exchange_small(
    n,
    head_tile,
    labels_hbm,
    emb_hbm,
    centers_ref,
    cbuf,
    lhs_ref,
    inv_ref,
    rhs_ref,
    fin_ref,
    sums_ref,
    head_ref,
    hat,
    hat_t,
    w_t,
    emb_ref,
    labels_ref,
    xall,
    lall,
    stat,
    stat_in,
    part,
    part_in,
    early_sums,
    sent,
    load_sem,
    small_sem,
    send_sem,
    recv_sem,
):
    me = lax.axis_index("cls")
    own, width = emb_ref.shape
    count = cbuf.shape[0]
    batch = n * own
    half = lanes // 2
    peers = [partner(me, n, k) for k in range(n - 1, 0, -1)]

    barrier = pltpu.get_barrier_semaphore()
    for peer in peers:
        pl.semaphore_signal(barrier, inc=1, device_id={"cls": peer}, device_id_type=MESH)

    small = [
        pltpu.make_async_copy(labels_hbm, labels_ref, small_sem.at[0]),
        pltpu.make_async_copy(emb_hbm, emb_ref, small_sem.at[1]),
    ]
    for copy in small:
        copy.start()
    def send(src, dst, kind, peer):
        pltpu.make_async_remote_copy(
            src_ref=src,
            dst_ref=dst,
            send_sem=send_sem.at[min(kind, 1)],
            recv_sem=recv_sem.at[kind],
            device_id={"cls": peer},
            device_id_type=MESH,
        ).start()

    def send_in_order(piece, into, kind):
        for j in range(n - 1):
            peer = j + (j >= me).astype(jnp.int32)
            send(piece(peer), into.at[me - (me > peer).astype(jnp.int32)], kind, peer)

    for copy in small:
        copy.wait()
    load = count // load_sem.shape[0]
    loads = []
    for k in range(count // load):
        at = pl.ds(k * load, load)
        copy = pltpu.make_async_copy(centers_ref.at[at], cbuf.at[at], load_sem.at[k])
        copy.start()
        loads.append(copy)

    lane = iota((own, lanes), 1)
    label_row = jnp.zeros((1, lanes), jnp.int32)
    for i in range(own):
        label_row = jnp.where(lane[:1] == i, labels_ref[i], label_row)
    lall[me] = label_row.astype(f32)
    x = emb_ref[...].astype(f32)
    xall[me] = (x * lax.rsqrt(jnp.sum(x * x, axis=1, keepdims=True) + norm_eps)).astype(bf16)

    pl.semaphore_wait(barrier, n - 1)
    for peer in peers:
        send(lall.at[me], lall.at[me], 3, peer)
        send(xall.at[me], xall.at[me], 0, peer)

    sub = largest_tile(load, 64)
    turn = largest_tile(load, 512)
    for k in range(count // load):
        loads[k].wait()
        for i in range(load // sub):
            at = pl.ds(k * load + i * sub, sub)
            c = cbuf[at, :].astype(f32)
            inverse = lax.rsqrt(jnp.sum(c * c, axis=1, keepdims=True) + norm_eps)
            inv_ref[at, :] = jnp.broadcast_to(inverse, (sub, lanes))
            hat[at, :] = (c * inverse).astype(bf16)
        for i in range(load // turn):
            at = pl.ds(k * load + i * turn, turn)
            hat_t[:, at] = hat[at, :].T

    total_wait(lall.at[pl.ds(0, n - 1)], recv_sem.at[3])
    total_wait(xall.at[pl.ds(0, n - 1)], recv_sem.at[0])

    x_hat = jnp.concatenate([xall[j] for j in range(n)], axis=0)
    diagonal = lane == iota((own, lanes), 0)
    labels = [jnp.sum(jnp.where(diagonal, lall[j], 0.0), axis=1, keepdims=True) for j in range(n)]
    label_col = jnp.concatenate(labels, axis=0).astype(jnp.int32) - me * count
    lane = iota((batch, lanes), 1)
    ahead = jnp.broadcast_to(label_col, (batch, lanes)) - lane
    tile = largest_tile(count, 256)
    blocks = range(tile // lanes)

    def one_hots(first, last):
        for k in range(first * tile, last * tile, lanes):
            at = pl.ds(k, lanes)
            one_hot = jnp.where(ahead == k, 1.0, 0.0).astype(bf16)
            w_t[batch : 2 * batch, at] = one_hot
            w_t[3 * batch :, at] = one_hot

    others = jnp.zeros((batch, lanes), f32)
    picked = jnp.zeros((batch, lanes), f32)
    for k in range(count // tile):
        wide_cosine = jnp.dot(
            x_hat, hat_t[:, k * tile : (k + 1) * tile], preferred_element_type=f32
        )
        for i in blocks:
            at = pl.ds(k * tile + i * lanes, lanes)
            cosine = wide_cosine[:, i * lanes : (i + 1) * lanes]
            mask = ahead == k * tile + i * lanes
            values = jnp.where(mask, 0.0, jnp.exp2((logit_scale * log2_e) * cosine))
            w_t[:batch, at] = values.astype(bf16)
            w_t[2 * batch : 3 * batch, at] = (values * cosine).astype(bf16)
            others = others + values
            picked = picked + jnp.where(mask, cosine, 0.0)
    early = count * 3 // 8
    one_hots(0, early // tile)
    early_sums[...] = jnp.dot(w_t[: 2 * batch, :early], hat[:early, :], preferred_element_type=f32)
    others = jnp.sum(others, axis=1, keepdims=True)
    picked = jnp.sum(picked, axis=1, keepdims=True)
    lane = lane[:own]
    mine = jnp.zeros((own, lanes), f32)
    for j in range(n):
        mine = jnp.where(lane == j, others[j * own : (j + 1) * own], mine)
        mine = jnp.where(lane == half + j, picked[j * own : (j + 1) * own], mine)
    stat[...] = mine
    for k, peer in enumerate(peers):
        send(stat, stat_in.at[k], 1, peer)

    total_wait(xall.at[pl.ds(0, n - 1)], send_sem.at[0])
    one_hots(early // tile, count // tile)
    summed = early_sums[...] + jnp.dot(
        w_t[: 2 * batch, early:], hat[early:, :], preferred_element_type=f32
    )
    for j in range(n):
        part[j] = jnp.concatenate(
            [summed[j * own : (j + 1) * own], summed[batch + j * own : batch + (j + 1) * own]],
            axis=0,
        ).astype(bf16)
    send_in_order(lambda peer: part.at[peer], part_in, 2)

    for k in range(count // tile):
        at = pl.ds(k * tile, tile)
        lhs_ref[at, :] = w_t[:, at].T

    total_wait(stat_in, recv_sem.at[1])
    sums = stat[...]
    for k in range(n - 1):
        sums = sums + stat_in[k]
    sums_ref[...] = sums
    _, slope, label_exp, label_weight = margin_terms(sums)

    def column(value, first):
        return jnp.concatenate(
            [
                jnp.broadcast_to(value[:, first + j : first + j + 1], (own, lanes))
                for j in range(n)
            ],
            axis=0,
        )

    others_col = column(sums, 0)
    exp_col, pull_col, weight_col, target_col = (
        column(v, half) for v in (label_exp, logit_scale * slope, label_weight, sums)
    )
    inverse_col = logit_scale / (others_col + exp_col)
    dot_col = (weight_col * inverse_col - pull_col) * target_col
    x_wide = x_hat.astype(f32)
    inverse_wide, pull_wide, weight_wide = (
        jnp.concatenate([v] * (width // lanes), axis=1)
        for v in (inverse_col, pull_col, weight_col)
    )
    scaled = (x_wide * inverse_wide).astype(bf16)
    label_term = weight_wide * scaled.astype(f32) - pull_wide * x_wide
    high = label_term.astype(bf16)
    low = (label_term - high.astype(f32)).astype(bf16)
    dot_high = dot_col.astype(bf16)
    dot_low = (dot_col - dot_high.astype(f32)).astype(bf16)
    rhs_ref[:, :width] = jnp.concatenate([scaled, high, jnp.zeros_like(high), low], axis=0)
    rhs_ref[:, width:] = jnp.concatenate(
        [jnp.zeros_like(dot_high), dot_high, inverse_col.astype(bf16), dot_low], axis=0
    )
    for k in range(head_ref.shape[0] // head_tile):
        at = pl.ds(k * head_tile, head_tile)
        head_ref[at, :] = gradient_tile(lhs_ref, inv_ref, cbuf, rhs_ref, at)

    total_wait(part_in, recv_sem.at[2])
    mine = part[me].astype(f32)
    for k in range(n - 1):
        mine = mine + part_in[k].astype(f32)
    fin_ref[...] = mine
    total_wait(sent, send_sem.at[1])


def gradient_kernel(
    tile,
    lhs_ref,
    inv_ref,
    centers_ref,
    rhs_ref,
    emb_ref,
    fin_ref,
    col_ref,
    head_ref,
    loss_hbm,
    emb_grad_hbm,
    grad_hbm,
    loss_buf,
    emb_grad_buf,
    grad_buf,
    sems,
):
    own, width = emb_ref.shape
    count = lhs_ref.shape[0]
    fused = rhs_ref.shape[1] > width
    steps = count // tile
    head = head_ref.shape[0] // tile
    for k in range(head):
        at = pl.ds(k * tile, tile)
        pltpu.make_async_copy(head_ref.at[at], grad_hbm.at[at], sems.at[0]).start()
    for k in range(head, steps):
        at = pl.ds(k * tile, tile)
        grad_buf[at, :] = gradient_tile(lhs_ref, inv_ref, centers_ref, rhs_ref, at)
        pltpu.make_async_copy(grad_buf.at[at], grad_hbm.at[at], sems.at[0]).start()
        if k == head:
            x = emb_ref[...].astype(f32)
            inverse = lax.rsqrt(jnp.sum(x * x, axis=1, keepdims=True) + norm_eps)
            units = x * inverse
            if fused:
                me = lax.axis_index("cls")
                lane = iota((own, lanes), 1)
                others, target_cos = (
                    jnp.sum(jnp.where(lane == at, col_ref[...], 0.0), axis=1, keepdims=True)
                    for at in (me, me + lanes // 2)
                )
                shifted, slope, label_exp, weight = margin_terms(target_cos)
                total = others + label_exp
                loss = jnp.log(total) - logit_scale * shifted
                total = total * (1.0 / logit_scale)
            else:
                total, slope, weight, loss = (col_ref[:, at : at + 1] for at in range(4))
            picked = fin_ref[own:, :]
            grad = (fin_ref[:own, :] + weight * picked) / total - (logit_scale * slope) * picked
            emb_grad_buf[...] = inverse * (
                grad - units * jnp.sum(units * grad, axis=1, keepdims=True)
            )
            diagonal = iota((own, lanes), 0) == iota((own, lanes), 1)
            loss_row = jnp.sum(jnp.where(diagonal, jnp.broadcast_to(loss, (own, lanes)), 0.0), axis=0, keepdims=True)
            loss_buf[...] = loss_row[:, :own]
        if k == min(head + 1, steps - 1):
            pltpu.make_async_copy(emb_grad_buf, emb_grad_hbm, sems.at[1]).start()
            pltpu.make_async_copy(loss_buf, loss_hbm, sems.at[2]).start()
    total_wait(grad_hbm, sems.at[0])
    total_wait(emb_grad_hbm, sems.at[1])
    total_wait(loss_hbm, sems.at[2])


def per_device(n, embeddings, labels, centers):
    own, width = embeddings.shape
    count = centers.shape[0]
    batch = n * own
    wide = 2 * batch
    vmem = pl.BlockSpec(memory_space=pltpu.VMEM)
    dma = pltpu.SemaphoreType.DMA
    load = largest_tile(count, 512)
    hbm = pl.BlockSpec(memory_space=pltpu.HBM)
    tile = largest_tile(count, 128)
    fused = wide == lanes
    head = tile * min(2, count // tile - 1)
    if fused:
        kernel = exchange_small
        scratch = [
            pltpu.VMEM((count, width), bf16),
            pltpu.VMEM((width, count), bf16),
            pltpu.VMEM((4 * batch, count), bf16),
            pltpu.VMEM((own, width), bf16),
            pltpu.SMEM((own,), jnp.int32),
            pltpu.VMEM((n, own, width), bf16),
            pltpu.VMEM((n, 1, lanes), f32),
            pltpu.VMEM((own, lanes), f32),
            pltpu.VMEM((n - 1, own, lanes), f32),
            pltpu.VMEM((n, 2 * own, width), bf16),
            pltpu.VMEM((n - 1, 2 * own, width), bf16),
            pltpu.VMEM((2 * batch, width), f32),
            pltpu.VMEM(((n - 1) * (1 + own + own * width // lanes), 1, lanes), f32),
            dma((2,)),
            dma((2,)),
            dma((2,)),
            dma((4,)),
        ]
    else:
        kernel = exchange_large
        scratch = [
            pltpu.VMEM((count, width), bf16),
            pltpu.VMEM((own, width), bf16),
            pltpu.SMEM((own,), jnp.int32),
            pltpu.VMEM((n, own, width), bf16),
            pltpu.VMEM((n, 1, wide), jnp.int32),
            pltpu.VMEM((1, wide), f32),
            pltpu.VMEM((n - 1, 1, wide), f32),
            pltpu.VMEM((n, 2 * own, width), bf16),
            pltpu.VMEM((n - 1, 2 * own, width), bf16),
            pltpu.VMEM((batch, lanes), f32),
            dma((count // load,)),
            dma((2,)),
        ] + [dma((n - 1,))] * 8
    cached, lhs, inv, rhs, fin, col, grad_head = pl.pallas_call(
        functools.partial(kernel, n, tile),
        out_shape=(
            jax.ShapeDtypeStruct((count, width), bf16),
            jax.ShapeDtypeStruct((count, 4 * batch if fused else wide), bf16),
            jax.ShapeDtypeStruct((count, lanes), f32),
            jax.ShapeDtypeStruct((4 * batch, width + lanes if fused else width), bf16),
            jax.ShapeDtypeStruct((2 * own, width), f32),
            jax.ShapeDtypeStruct((own, lanes), f32),
            jax.ShapeDtypeStruct((head, width), f32),
        ),
        in_specs=[hbm, hbm, hbm],
        out_specs=(vmem,) * 7,
        scratch_shapes=scratch,
        compiler_params=pltpu.CompilerParams(
            collective_id=0, has_side_effects=True, vmem_limit_bytes=40 * 2**20
        ),
        name="exchange",
    )(*(pltpu.with_memory_space_constraint(v, pltpu.HBM) for v in (labels, embeddings, centers)))

    losses, emb_grad, center_grad = pl.pallas_call(
        functools.partial(gradient_kernel, tile),
        out_shape=(
            jax.ShapeDtypeStruct((1, own), f32),
            jax.ShapeDtypeStruct((own, width), f32),
            jax.ShapeDtypeStruct((count, width), f32),
        ),
        in_specs=[vmem] * 8,
        out_specs=(hbm,) * 3,
        scratch_shapes=[
            pltpu.VMEM((1, own), f32),
            pltpu.VMEM((own, width), f32),
            pltpu.VMEM((count, width), f32),
            dma((3,)),
        ],
        compiler_params=pltpu.CompilerParams(vmem_limit_bytes=32 * 2**20),
        name="gradient",
    )(lhs, inv, cached, rhs, embeddings, fin, col, grad_head)
    return losses.reshape(own), emb_grad, center_grad


def solution(mesh):
    in_specs = (P(("dp", "cls"), None), P(("dp", "cls")), P(("dp", "cls"), None))
    out_specs = (P(("dp", "cls")), P(("dp", "cls"), None), P(("dp", "cls"), None))
    return jax.shard_map(
        functools.partial(per_device, mesh.shape["cls"]),
        mesh=mesh,
        in_specs=in_specs,
        out_specs=out_specs,
        check_vma=False,
    )
```
